256 devices in a mesh: row: 32 (over x_hi, z, core), col: 8 (over x_lo, y).
Axes of the slice: x: 4 (x_hi: 2, x_lo: 2; x = x_hi * 2 + x_lo), y: 4, z: 8, core: 2. Of those that a mesh axis runs over, the one named last changes fastest.
Arguments:
- occupied_waves: bfloat16 [1024, 32768], P('row', 'col'), may hold values from -6 to 6
- virtual_waves: bfloat16 [512, 32768], P('row', 'col'), may hold values from -6 to 6
- occupied_decay: float32 [1024], replicated, may hold values from 0.02 to 1
- virtual_decay: float32 [512], replicated, may hold values from 0.02 to 1
Outputs:
- spectrum_real: float32 [1024, 32, 1024], P('row', 'col')
- spectrum_imaginary: float32 [1024, 32, 1024], P('row', 'col')
The draws below stay inside these ranges and needn't reach their ends.
All inputs are finite; a program needn't handle non-finite values.
Results may differ from the reference program's by a relative error of at most 0.0041.
Values may be sent and summed in bfloat16 or wider, within the bound.
No kernel may reach another device: no remote copies, remote signals or barrier semaphores. Data moves between devices by JAX's collectives and lax.ppermute only.
A program may use at most 64 MiB of HBM per device.

```python
import math
import jax
import jax.numpy as jnp
from jax import lax

NOCC = 1024
NVIR = 512
NA = 32
NB = 32
NC = 32
ROWS_DEV = 32
NGRID = 32768
N_ROW = 32


def steps_of(key, dims, pieces, smallest, high):
    loudness, own = 1.0, jax.random.fold_in(key, 6)
    for position, parts in pieces:
        heights = jnp.exp(jax.random.uniform(jax.random.fold_in(own, position), (parts,), jnp.float32, smallest / len(pieces), high / len(pieces)))
        loudness = loudness * jnp.repeat(heights, dims[position] // parts).reshape([-1 if axis == position else 1 for axis in range(len(dims))])
    return loudness


def noise(rng, extent, scale, limit, split=(), kind=jnp.bfloat16):
    drawn = scale * jax.random.normal(rng, extent, jnp.float32)
    if split:
        drawn = drawn * steps_of(rng, extent, split, -0.22, 0.18)
    return jnp.clip(drawn, -limit, limit).astype(kind)


def setup_inputs(seed: int = 0) -> dict:
    keys = jax.random.split(jax.random.key(seed), 5)
    return {
        "occupied_waves": noise(keys[0], (NOCC, NGRID), 1.0, 6.0, ((0, 32), (1, 8))),
        "virtual_waves": noise(keys[1], (NVIR, NGRID), 1.0, 6.0, ((0, 32), (1, 8))),
        "occupied_decay": jnp.clip(jnp.exp(jax.random.uniform(keys[2], (NOCC,), jnp.float32, math.log(0.02), math.log(1.0))), 0.02, 1.0),
        "virtual_decay": jnp.clip(jnp.exp(jax.random.uniform(keys[3], (NVIR,), jnp.float32, math.log(0.02), math.log(1.0))), 0.02, 1.0),
    }


def reference(occupied_waves, virtual_waves, occupied_decay, virtual_decay):
    rows_all = ROWS_DEV * N_ROW
    width = math.gcd(rows_all, 512)
    factor = -1.0 / math.sqrt(NOCC * NVIR)
    contract = (((0,), (0,)), ((), ()))

    def block(index):
        first = (index * width).astype(jnp.int32)
        occ_rows = lax.dynamic_slice_in_dim(occupied_waves, first, width, 1)
        occ_rows = (occ_rows.astype(jnp.float32) * occupied_decay[:, None]).astype(jnp.bfloat16)
        vir_rows = lax.dynamic_slice_in_dim(virtual_waves, first, width, 1)
        vir_rows = (vir_rows.astype(jnp.float32) * virtual_decay[:, None]).astype(jnp.bfloat16)
        green_occ = lax.dot_general(occupied_waves, occ_rows, contract, preferred_element_type=jnp.float32)
        green_vir = lax.dot_general(virtual_waves, vir_rows, contract, preferred_element_type=jnp.float32)
        polar = green_occ * green_vir * factor
        cube = polar.reshape(NA, NB, NC, width)
        spectrum = jnp.fft.fftn(cube, axes=(0, 1, 2)) / math.sqrt(NGRID)
        spectrum = jnp.transpose(spectrum, (3, 2, 0, 1)).reshape(width, NC, NA * NB)
        return (jnp.real(spectrum).astype(jnp.float32), jnp.imag(spectrum).astype(jnp.float32))
    real_part, imag_part = lax.map(block, jnp.arange(rows_all // width, dtype=jnp.int32))
    real_part = real_part.reshape(rows_all, NC, NA * NB)
    imag_part = imag_part.reshape(rows_all, NC, NA * NB)
    return (real_part, imag_part)
```

```python
import math

import jax
import jax.numpy as jnp
import numpy as np
from jax import lax
from jax.experimental import pallas as pl
from jax.experimental.pallas import tpu as pltpu
from jax.sharding import Mesh, PartitionSpec as P

NOCC = 1024
NVIR = 512
NGRID = 32768
POLAR_FACTOR = -1.0 / math.sqrt(NOCC * NVIR)
NORMAL = 1.0 / math.sqrt(NGRID)
FINE = ("xh", "z", "c", "xl", "y")
FINE_SIZES = (2, 8, 2, 2, 4)
ROW = ("xh", "z", "c")
COL = ("xl", "y")
SAME_CORE = ("xh", "z", "xl", "y")
BF16 = jnp.bfloat16
F32 = jnp.float32


def split_table(table):
    high = table.astype(np.float32).astype(jnp.bfloat16)
    low = (table - high.astype(np.float64)).astype(np.float32).astype(jnp.bfloat16)
    return high, low


def rotation(phase):
    cosine, sine = np.cos(phase), np.sin(phase)
    return np.array([[cosine, sine], [-sine, cosine]])


def c_table():
    kc = np.arange(32).reshape(8, 4)
    turn = rotation(2 * np.pi * (kc[..., None] * np.arange(32) % 32) / 32)[:, 0]
    full = np.einsum("pjic,bd->ijpbdc", turn, np.eye(8))
    return split_table(full.reshape(512, 256))


def a_table():
    ka = np.arange(32)
    turn = rotation(2 * np.pi * (ka[:, None] * ka[None, :] % 32) / 32)
    turn = turn.reshape(2, 2, 8, 4, 8, 4)
    full = np.einsum("pqghck,bd->ghpbkcqd", turn, np.eye(8))
    return split_table(full.reshape(512, 512))


def b_table():
    kb = np.arange(32)
    turn = rotation(2 * np.pi * (kb[:, None] * kb[None, :] % 32) / 32) * NORMAL
    turn = turn.reshape(2, 2, 32, 4, 8)
    full = np.einsum("pqkBb,hj->Bhqbpjk", turn, np.eye(4))
    return split_table(full.reshape(256, 256))


def dot(a, b):
    return lax.dot_general(a, b, (((1,), (0,)), ((), ())), preferred_element_type=F32)


def prepare_kernel(place_ref, occ_decay_ref, vir_decay_ref, occ_ref, vir_ref, out_ref):
    row = place_ref[0]

    def column(decay_ref, count):
        index = lax.broadcasted_iota(jnp.int32, (count, 128), 0)
        out = jnp.zeros((count, 128), F32)
        for i in range(count):
            out = jnp.where(index == i, decay_ref[row * count + i], out)
        return out

    def chunks(ref, decay):
        count = ref.shape[0]
        scaled = [
            ref[:, 128 * t : 128 * (t + 1)].astype(F32) * decay for t in range(8)
        ]
        for y in range(4):
            first, second = scaled[2 * y], scaled[2 * y + 1]
            for h in range(2):
                pieces = [
                    part[:, 64 * u + 32 * h : 64 * u + 32 * h + 32]
                    for part in (first, second)
                    for u in range(2)
                ]
                yield y, h, jnp.concatenate(pieces, axis=1)

    for y, h, rows in chunks(occ_ref, column(occ_decay_ref, 32)):
        for xl in range(2):
            out_ref[4 * xl + y, h, 0:16, :] = rows[16 * xl : 16 * xl + 16].astype(BF16)
    for y, h, rows in chunks(vir_ref, column(vir_decay_ref, 16)):
        for xl in range(2):
            out_ref[4 * xl + y, h, 16:24, :] = rows[8 * xl : 8 * xl + 8].astype(BF16)


def prepare(place, occ_decay, vir_decay, occ, vir):
    smem = pl.BlockSpec(memory_space=pltpu.SMEM)
    return pl.pallas_call(
        prepare_kernel,
        grid=(1,),
        out_shape=jax.ShapeDtypeStruct((8, 2, 24, 128), BF16),
        in_specs=[
            smem,
            smem,
            smem,
            pl.BlockSpec((32, 1024), lambda i: (0, 0)),
            pl.BlockSpec((16, 1024), lambda i: (0, 0)),
        ],
        out_specs=pl.BlockSpec((8, 2, 24, 128), lambda i: (0, 0, 0, 0)),
        name="prepare",
    )(place, occ_decay, vir_decay, occ, vir)


def pack_kernel(occ_ref, vir_ref, rows_ref, out_ref):
    for p in range(32):
        out_ref[p, 0:32, :] = occ_ref[:, 128 * p : 128 * (p + 1)]
        out_ref[p, 32:48, :] = vir_ref[:, 128 * p : 128 * (p + 1)]
        out_ref[p, 48:72, :] = rows_ref[0, p % 2]


def pack(occ, vir, rows):
    return pl.pallas_call(
        pack_kernel,
        grid=(1,),
        out_shape=jax.ShapeDtypeStruct((32, 72, 128), BF16),
        in_specs=[
            pl.BlockSpec((32, 4096), lambda i: (0, 0)),
            pl.BlockSpec((16, 4096), lambda i: (0, 0)),
            pl.BlockSpec((1, 2, 24, 128), lambda i: (0, 0, 0, 0)),
        ],
        out_specs=pl.BlockSpec((32, 72, 128), lambda i: (0, 0, 0)),
        name="pack",
    )(occ, vir, rows)


def polar_kernel(core_ref, own_ref, other_ref, rows_ref, high_ref, low_ref, out_ref, polar_ref):
    core = core_ref[0]
    for half, ref in enumerate((own_ref, other_ref)):
        start = pl.multiple_of((core if half == 0 else 1 - core) * 128, 128)
        occ = ref[0:1024, :].T
        vir = ref[1024:1536, :].T
        for y in range(4):
            green_occ = dot(occ[:, :512], rows_ref[y, :512]) + dot(
                occ[:, 512:], rows_ref[4 + y, :512]
            )
            green_vir = dot(vir[:, :256], rows_ref[y, 512:]) + dot(
                vir[:, 256:], rows_ref[4 + y, 512:]
            )
            polar_ref[pl.ds(start, 128), 128 * y : 128 * (y + 1)] = (
                green_occ * green_vir * POLAR_FACTOR
            )
    polar = polar_ref[...]
    polar_high = polar.astype(BF16)
    polar_low = (polar - polar_high.astype(F32)).astype(BF16)
    spectrum = (
        dot(high_ref[...], polar_high)
        + dot(high_ref[...], polar_low)
        + dot(low_ref[...], polar_high)
    )
    for m in range(16):
        pieces = [spectrum[128 * i : 128 * (i + 1), 32 * m : 32 * (m + 1)] for i in range(4)]
        out_ref[m] = jnp.concatenate(pieces, axis=1).astype(BF16)


def polar_messages(core, own, other, rows):
    high, low = c_table()
    vmem = pl.BlockSpec(memory_space=pltpu.VMEM)
    return pl.pallas_call(
        polar_kernel,
        out_shape=jax.ShapeDtypeStruct((16, 128, 128), BF16),
        in_specs=[pl.BlockSpec(memory_space=pltpu.SMEM)] + [vmem] * 5,
        out_specs=vmem,
        scratch_shapes=[pltpu.VMEM((256, 512), F32)],
        name="polar",
    )(core, own, other, rows, high, low)


def finish_kernel(x_ref, a_high_ref, a_low_ref, b_high_ref, b_low_ref, real_ref, imag_ref):
    planes = []
    for block in range(4):
        x = jnp.concatenate(
            [x_ref[128 * (4 * k + block) : 128 * (4 * k + block + 1), :] for k in range(4)], axis=0
        )
        planes.append(dot(a_high_ref[...], x) + dot(a_low_ref[...], x))
    for g in range(8):
        z = jnp.concatenate([plane[64 * g : 64 * (g + 1)] for plane in planes], axis=0).T
        z_high = z.astype(BF16)
        z_low = (z - z_high.astype(F32)).astype(BF16)
        out = (
            dot(z_high, b_high_ref[...])
            + dot(z_high, b_low_ref[...])
            + dot(z_low, b_high_ref[...])
        )
        for i in range(4):
            real_ref[:, i, 128 * g : 128 * (g + 1)] = out[32 * i : 32 * (i + 1), :128]
            imag_ref[:, i, 128 * g : 128 * (g + 1)] = out[32 * i : 32 * (i + 1), 128:]


def finish(x):
    vmem = pl.BlockSpec(memory_space=pltpu.VMEM)
    shape = jax.ShapeDtypeStruct((32, 4, 1024), F32)
    return pl.pallas_call(
        finish_kernel,
        out_shape=(shape, shape),
        in_specs=[vmem] * 5,
        out_specs=(vmem, vmem),
        name="finish",
    )(x, *a_table(), *b_table())


def on_device(occ, vir, occ_decay, vir_decay):
    row = lax.axis_index(ROW).astype(jnp.int32).reshape(1)
    core = lax.axis_index("c").astype(jnp.int32).reshape(1)
    scattered = lax.all_to_all(prepare(row, occ_decay, vir_decay, occ, vir), COL, 0, 0, tiled=True)
    arrived = lax.all_to_all(pack(occ, vir, scattered), ROW, 0, 0, tiled=True)

    def by_half(part, count):
        part = part.reshape(32, 2, count // 2, 128)
        return jnp.transpose(part, (1, 0, 2, 3)).reshape(32 * count, 128)

    own = jnp.concatenate([by_half(arrived[:, :32], 32), by_half(arrived[:, 32:48], 16)], axis=0)
    share = jnp.concatenate(
        [arrived[:, 48:64].reshape(512, 128), arrived[:, 64:72].reshape(256, 128)], axis=0
    )
    other = lax.ppermute(own, "c", [(0, 1), (1, 0)])
    rows = lax.all_to_all(jnp.broadcast_to(share[None], (8, 768, 128)), COL, 0, 0, tiled=True)
    messages = polar_messages(core, own, other, rows).reshape(128, 16, 128)
    received = lax.all_to_all(messages, SAME_CORE, 0, 0, tiled=True)
    return finish(received.reshape(2048, 128))


def solution(mesh):
    fine = Mesh(mesh.devices.reshape(FINE_SIZES), FINE)
    return jax.shard_map(
        on_device,
        mesh=fine,
        in_specs=(P(ROW, COL), P(ROW, COL), P(), P()),
        out_specs=(P(ROW, COL, None), P(ROW, COL, None)),
        check_vma=False,
    )
```

```python
import math

import jax
import jax.numpy as jnp
import numpy as np
from jax import lax
from jax.experimental import pallas as pl
from jax.experimental.pallas import tpu as pltpu
from jax.sharding import Mesh, PartitionSpec as P

NOCC = 1024
NVIR = 512
NGRID = 32768
POLAR_FACTOR = -1.0 / math.sqrt(NOCC * NVIR)
NORMAL = 1.0 / math.sqrt(NGRID)
Z = ("z2", "z1", "z0")
Y = ("y1", "y0")
ROW = ("xh", *Z, "c")
COL = ("xl", *Y)
FINE = ROW + COL
LAST = ("z0", "y0", "y1", "z1", "xh", "xl", "z2")
BF16 = jnp.bfloat16
LIMIT = 16 * 1024 * 1024


def place_in_last(m, j):
    bits = dict(zip(("xh", *Z), ((m >> 3) & 1, (m >> 2) & 1, (m >> 1) & 1, m & 1)))
    bits.update(zip(COL, ((j >> 2) & 1, (j >> 1) & 1, j & 1)))
    place = 0
    for axis in LAST:
        place = 2 * place + bits[axis]
    return place


F32 = jnp.float32


def split_table(table):
    high = table.astype(np.float32).astype(jnp.bfloat16)
    low = (table - high.astype(np.float64)).astype(np.float32).astype(jnp.bfloat16)
    return high, low


def rotation(phase):
    cosine, sine = np.cos(phase), np.sin(phase)
    return np.array([[cosine, sine], [-sine, cosine]])


def c_table():
    kc = np.arange(32).reshape(8, 4)
    turn = rotation(2 * np.pi * (kc[..., None] * np.arange(32) % 32) / 32)[:, 0]
    full = np.einsum("pjic,bd->ijpbdc", turn, np.eye(8))
    return split_table(full.reshape(512, 256))


def a_table():
    ka = np.arange(32)
    turn = rotation(2 * np.pi * (ka[:, None] * ka[None, :] % 32) / 32)
    turn = turn.reshape(2, 2, 8, 4, 8, 4)
    full = np.einsum("pqghck,bd->ghpbkcqd", turn, np.eye(8))
    return split_table(full.reshape(512, 512))


def b_table():
    kb = np.arange(32)
    turn = rotation(2 * np.pi * (kb[:, None] * kb[None, :] % 32) / 32) * NORMAL
    turn = turn.reshape(2, 2, 32, 4, 8)
    full = np.einsum("pqkBb,hj->Bhqbpjk", turn, np.eye(4))
    return split_table(full.reshape(256, 256))


def dot(a, b):
    return lax.dot_general(a, b, (((1,), (0,)), ((), ())), preferred_element_type=F32)


def prepare_kernel(place_ref, occ_decay_ref, vir_decay_ref, occ_ref, vir_ref, out_ref):
    row = place_ref[0]

    def column(decay_ref, count):
        index = lax.broadcasted_iota(jnp.int32, (count, 128), 0)
        out = jnp.zeros((count, 128), F32)
        for i in range(count):
            out = jnp.where(index == i, decay_ref[row * count + i], out)
        return out

    def chunks(ref, decay):
        count = ref.shape[0]
        scaled = [
            ref[:, 128 * t : 128 * (t + 1)].astype(F32) * decay for t in range(8)
        ]
        for y in range(4):
            first, second = scaled[2 * y], scaled[2 * y + 1]
            for h in range(2):
                pieces = [
                    part[:, 64 * u + 32 * h : 64 * u + 32 * h + 32]
                    for part in (first, second)
                    for u in range(2)
                ]
                yield y, h, jnp.concatenate(pieces, axis=1)

    for y, h, rows in chunks(occ_ref, column(occ_decay_ref, 32)):
        for xl in range(2):
            out_ref[4 * xl + y, h, 0:16, :] = rows[16 * xl : 16 * xl + 16].astype(BF16)
    for y, h, rows in chunks(vir_ref, column(vir_decay_ref, 16)):
        for xl in range(2):
            out_ref[4 * xl + y, h, 16:24, :] = rows[8 * xl : 8 * xl + 8].astype(BF16)


def prepare(place, occ_decay, vir_decay, occ, vir):
    smem = pl.BlockSpec(memory_space=pltpu.SMEM)
    return pl.pallas_call(
        prepare_kernel,
        grid=(1,),
        out_shape=jax.ShapeDtypeStruct((8, 2, 24, 128), BF16),
        in_specs=[
            smem,
            smem,
            smem,
            pl.BlockSpec((32, 1024), lambda i: (0, 0)),
            pl.BlockSpec((16, 1024), lambda i: (0, 0)),
        ],
        out_specs=pl.BlockSpec((8, 2, 24, 128), lambda i: (0, 0, 0, 0)),
        name="prepare",
    )(place, occ_decay, vir_decay, occ, vir)


def pack_kernel(occ_ref, vir_ref, out_ref):
    for p in range(32):
        out_ref[p, 0:32, :] = occ_ref[:, 128 * p : 128 * (p + 1)]
        out_ref[p, 32:48, :] = vir_ref[:, 128 * p : 128 * (p + 1)]


def pack(occ, vir):
    vmem = pl.BlockSpec(memory_space=pltpu.VMEM)
    return pl.pallas_call(
        pack_kernel,
        out_shape=jax.ShapeDtypeStruct((32, 48, 128), BF16),
        in_specs=[vmem, vmem],
        out_specs=vmem,
        compiler_params=pltpu.CompilerParams(vmem_limit_bytes=LIMIT),
        name="pack",
    )(occ, vir)


def polar_kernel(place_ref, own_ref, other_ref, near_ref, *refs):
    step_refs, (up_ref, down_ref, high_ref, low_ref, out_ref, polar_ref) = refs[:3], refs[3:]
    core, xl, y = place_ref[0], place_ref[1], place_ref[2]
    near = (near_ref, *step_refs)
    points = []
    for ref in (own_ref, other_ref):
        halves = []
        for half in (xl, 1 - xl):
            occ = ref[pl.ds(pl.multiple_of(half * 512, 512), 512), :].T
            vir = ref[pl.ds(pl.multiple_of(1024 + half * 256, 256), 256), :].T
            halves.append((occ, vir))
        points.append(halves)
    for step in range(4):
        far_ref = up_ref if step < 2 else down_ref
        base = 768 * (step % 2)
        for which, halves in enumerate(points):
            start = pl.multiple_of((core if which == 0 else 1 - core) * 128, 128)
            (occ_near, vir_near), (occ_far, vir_far) = halves
            green_occ = dot(occ_near, near[step][:512]) + dot(occ_far, far_ref[base : base + 512])
            green_vir = dot(vir_near, near[step][512:]) + dot(
                vir_far, far_ref[base + 512 : base + 768]
            )
            polar_ref[pl.ds(start, 128), 128 * step : 128 * (step + 1)] = (
                green_occ * green_vir * POLAR_FACTOR
            )
    polar = polar_ref[...]
    polar_high = polar.astype(BF16)
    polar_low = (polar - polar_high.astype(F32)).astype(BF16)
    spectrum = (
        dot(high_ref[...], polar_high)
        + dot(high_ref[...], polar_low)
        + dot(low_ref[...], polar_high)
    )
    for step in range(4):
        chunk = lax.rem(y + 4 - step, 4)
        for u in range(4):
            lane = 128 * step + 32 * u
            pieces = [spectrum[128 * i : 128 * (i + 1), lane : lane + 32] for i in range(4)]
            out_ref[4 * chunk + u] = jnp.concatenate(pieces, axis=1).astype(BF16)


def polar_messages(place, *arrays):
    high, low = c_table()
    vmem = pl.BlockSpec(memory_space=pltpu.VMEM)
    return pl.pallas_call(
        polar_kernel,
        out_shape=jax.ShapeDtypeStruct((16, 128, 128), BF16),
        in_specs=[pl.BlockSpec(memory_space=pltpu.SMEM)] + [vmem] * 10,
        out_specs=vmem,
        scratch_shapes=[pltpu.VMEM((256, 512), F32)],
        compiler_params=pltpu.CompilerParams(vmem_limit_bytes=LIMIT),
        name="polar",
    )(place, *arrays, high, low)


def finish_kernel(x_ref, a_high_ref, a_low_ref, b_high_ref, b_low_ref, real_ref, imag_ref):
    planes = []
    for block in range(4):
        x = jnp.concatenate(
            [x_ref[128 * (4 * k + block) : 128 * (4 * k + block + 1), :] for k in range(4)], axis=0
        )
        planes.append(dot(a_high_ref[...], x) + dot(a_low_ref[...], x))
    for g in range(8):
        z = jnp.concatenate([plane[64 * g : 64 * (g + 1)] for plane in planes], axis=0).T
        z_high = z.astype(BF16)
        z_low = (z - z_high.astype(F32)).astype(BF16)
        out = (
            dot(z_high, b_high_ref[...])
            + dot(z_high, b_low_ref[...])
            + dot(z_low, b_high_ref[...])
        )
        for i in range(4):
            real_ref[:, i, 128 * g : 128 * (g + 1)] = out[32 * i : 32 * (i + 1), :128]
            imag_ref[:, i, 128 * g : 128 * (g + 1)] = out[32 * i : 32 * (i + 1), 128:]


def finish(x):
    vmem = pl.BlockSpec(memory_space=pltpu.VMEM)
    shape = jax.ShapeDtypeStruct((32, 4, 1024), F32)
    return pl.pallas_call(
        finish_kernel,
        out_shape=(shape, shape),
        in_specs=[vmem] * 5,
        out_specs=(vmem, vmem),
        compiler_params=pltpu.CompilerParams(vmem_limit_bytes=LIMIT),
        name="finish",
    )(x, *a_table(), *b_table())


def shift(x, axes, count, by):
    return lax.ppermute(x, axes, [(i, (i + by) % count) for i in range(count)])


def on_device(occ, vir, occ_decay, vir_decay):
    row = lax.axis_index(ROW).astype(jnp.int32).reshape(1)
    place = jnp.stack([lax.axis_index(a).astype(jnp.int32) for a in ("c", "xl", Y)])
    scattered = lax.all_to_all(prepare(row, occ_decay, vir_decay, occ, vir), COL, 0, 0, tiled=True)
    share = jnp.broadcast_to(scattered[0][None], (16, 2, 24, 128)).reshape(32, 24, 128)
    share = lax.all_to_all(share, ROW, 0, 0, tiled=True)
    arrived = lax.all_to_all(pack(occ, vir), ROW, 0, 0, tiled=True)

    near = jnp.concatenate([share[:, :16].reshape(512, 128), share[:, 16:].reshape(256, 128)], axis=0)
    steps = [shift(near, Y, 4, by) for by in (1, 2, 3)]
    up = shift(jnp.concatenate([near, steps[0]], axis=0), ("xh", "xl"), 4, 1)
    down = shift(jnp.concatenate([steps[1], steps[2]], axis=0), ("xh", "xl"), 4, -1)

    def by_half(part, count):
        part = part.reshape(32, 2, count // 2, 128)
        return jnp.transpose(part, (1, 0, 2, 3)).reshape(32 * count, 128)

    own = jnp.concatenate([by_half(arrived[:, :32], 32), by_half(arrived[:, 32:], 16)], axis=0)
    other = lax.ppermute(own, "c", [(0, 1), (1, 0)])
    messages = polar_messages(place, own, other, near, *steps, up, down).reshape(16, 8, 16, 128)

    bits = messages.reshape(2, 2, 2, 2, 2, 2, 2, 16, 128)
    names = ("xh", *Z, *COL)
    to_last = [names.index(a) for a in LAST]
    sent = jnp.transpose(bits, (*to_last, 7, 8)).reshape(128, 16, 128)
    received = lax.all_to_all(sent, LAST, 0, 0, tiled=True).reshape(bits.shape)
    back = [LAST.index(a) for a in names]
    return finish(jnp.transpose(received, (*back, 7, 8)).reshape(2048, 128))


def solution(mesh):
    fine = Mesh(mesh.devices.reshape((2,) * len(FINE)), FINE)
    return jax.shard_map(
        on_device,
        mesh=fine,
        in_specs=(P(ROW, COL), P(ROW, COL), P(), P()),
        out_specs=(P(ROW, COL, None), P(ROW, COL, None)),
        check_vma=False,
    )
```

```python
import math

import jax
import jax.numpy as jnp
import numpy as np
from jax import lax
from jax.experimental import pallas as pl
from jax.experimental.pallas import tpu as pltpu
from jax.sharding import Mesh, PartitionSpec as P


NOCC = 1024
NVIR = 512
NGRID = 32768
POLAR_FACTOR = -1.0 / math.sqrt(NOCC * NVIR)
NORMAL = 1.0 / math.sqrt(NGRID)
Z = ("z2", "z1", "z0")
Y = ("y1", "y0")
ROW = ("xh", *Z, "c")
COL = ("xl", *Y)
FINE = ROW + COL
LAST = ("z1", "xl", "y0", "z2", "xh", "y1")
BF16 = jnp.bfloat16
F32 = jnp.float32
LIMIT = 16 * 1024 * 1024


def split_table(table):
    high = table.astype(np.float32).astype(jnp.bfloat16)
    low = (table - high.astype(np.float64)).astype(np.float32).astype(jnp.bfloat16)
    return high, low


def rotation(phase):
    cosine, sine = np.cos(phase), np.sin(phase)
    return np.array([[cosine, sine], [-sine, cosine]])


def c_table():
    kc = np.arange(32).reshape(8, 4)
    turn = rotation(2 * np.pi * (kc[..., None] * np.arange(32) % 32) / 32)[:, 0]
    full = np.einsum("pjic,bd->ijpbdc", turn, np.eye(8))
    return split_table(full.reshape(512, 256))


def a_table():
    ka = np.arange(32)
    turn = rotation(2 * np.pi * (ka[:, None] * ka[None, :] % 32) / 32)
    turn = turn.reshape(2, 2, 8, 4, 8, 4)
    full = np.einsum("pqghck,bd->ghpbkcqd", turn, np.eye(8))
    return split_table(full.reshape(512, 512))


def b_table():
    kb = np.arange(32)
    turn = rotation(2 * np.pi * (kb[:, None] * kb[None, :] % 32) / 32) * NORMAL
    turn = turn.reshape(2, 2, 32, 4, 8)
    full = np.einsum("pqkBb,hj->Bhqbpjk", turn, np.eye(4))
    return split_table(full.reshape(256, 256))


def dot(a, b):
    return lax.dot_general(a, b, (((1,), (0,)), ((), ())), preferred_element_type=F32)


def prepare_kernel(place_ref, occ_decay_ref, vir_decay_ref, occ_ref, vir_ref, out_ref):
    row = place_ref[0]

    def column(decay_ref, count):
        index = lax.broadcasted_iota(jnp.int32, (count, 128), 0)
        out = jnp.zeros((count, 128), F32)
        for i in range(count):
            out = jnp.where(index == i, decay_ref[row * count + i], out)
        return out

    def scaled_tiles(ref, decay):
        tiles = [ref[:, 128 * t : 128 * (t + 1)].astype(F32) * decay for t in range(8)]
        return [
            [
                jnp.concatenate(
                    [tiles[4 * t + u][:, 32 * kind : 32 * (kind + 1)] for u in range(4)], axis=1
                )
                for kind in range(4)
            ]
            for t in range(2)
        ]

    occ = scaled_tiles(occ_ref, column(occ_decay_ref, 32))
    vir = scaled_tiles(vir_ref, column(vir_decay_ref, 16))
    for xl in range(2):
        for y1 in range(2):
            for t in range(2):
                for kind in range(4):
                    group = 2 * xl + y1
                    piece = jnp.concatenate(
                        [
                            occ[t][kind][8 * group : 8 * (group + 1)],
                            vir[t][kind][8 * y1 : 8 * (y1 + 1)],
                        ],
                        axis=0,
                    )
                    out_ref[4 * xl + 2 * y1 + t, kind] = piece.astype(BF16)


def prepare(place, occ_decay, vir_decay, occ, vir):
    smem = pl.BlockSpec(memory_space=pltpu.SMEM)
    return pl.pallas_call(
        prepare_kernel,
        grid=(1,),
        out_shape=jax.ShapeDtypeStruct((8, 4, 16, 128), BF16),
        in_specs=[
            smem,
            smem,
            smem,
            pl.BlockSpec((32, 1024), lambda i: (0, 0)),
            pl.BlockSpec((16, 1024), lambda i: (0, 0)),
        ],
        out_specs=pl.BlockSpec((8, 4, 16, 128), lambda i: (0, 0, 0, 0)),
        name="prepare",
    )(place, occ_decay, vir_decay, occ, vir)


def pack_kernel(occ_ref, vir_ref, rows_ref, out_ref):
    for p in range(32):
        out_ref[p, 0:32, :] = occ_ref[:, 128 * p : 128 * (p + 1)]
        out_ref[p, 32:48, :] = vir_ref[:, 128 * p : 128 * (p + 1)]
        out_ref[p, 48:64, :] = rows_ref[0, p % 4]


def pack(occ, vir, rows):
    vmem = pl.BlockSpec(memory_space=pltpu.VMEM)
    return pl.pallas_call(
        pack_kernel,
        out_shape=jax.ShapeDtypeStruct((32, 64, 128), BF16),
        in_specs=[vmem] * 3,
        out_specs=vmem,
        compiler_params=pltpu.CompilerParams(vmem_limit_bytes=LIMIT),
        name="pack",
    )(occ, vir, rows)


def polar_kernel(place_ref, *refs):
    points, near, far = refs[:4], refs[4:8], refs[8:10]
    high_ref, low_ref, out_ref, polar_ref, occ_ref, vir_ref = refs[10:]
    core, z0, xl, y = place_ref[0], place_ref[1], place_ref[2], place_ref[3]
    for step in range(4):
        chunk = lax.rem(y + 4 - step, 4)
        y1, y0 = lax.div(chunk, 2), lax.rem(chunk, 2)
        lanes = pl.ds(pl.multiple_of(128 * y0, 128), 128)

        def rows(group):
            return pl.ds(pl.multiple_of(256 * group, 256), 256)

        occ_ref[rows(2 * xl + y1), lanes] = near[step][:256]
        occ_ref[rows(2 * (1 - xl) + y1), lanes] = far[step // 2][
            256 * (step % 2) : 256 * (step % 2 + 1)
        ]
        vir_ref[rows(y1), lanes] = near[step][256:]
    for k, ref in enumerate(points):
        place = 2 * (z0 if k < 2 else 1 - z0) + (core if k % 2 == 0 else 1 - core)
        green_occ = dot(ref[:1024].T, occ_ref[...])
        green_vir = dot(ref[1024:].T, vir_ref[...])
        polar_ref[pl.ds(pl.multiple_of(128 * place, 128), 128), :] = (
            green_occ * green_vir * POLAR_FACTOR
        )
    for half in range(2):
        polar = polar_ref[256 * half : 256 * (half + 1), :]
        polar_high = polar.astype(BF16)
        polar_low = (polar - polar_high.astype(F32)).astype(BF16)
        spectrum = (
            dot(high_ref[...], polar_high)
            + dot(high_ref[...], polar_low)
            + dot(low_ref[...], polar_high)
        )
        for m in range(8):
            pieces = [spectrum[128 * i : 128 * (i + 1), 32 * m : 32 * (m + 1)] for i in range(4)]
            message = jnp.concatenate(pieces, axis=1).astype(BF16)
            out_ref[m, :, half] = message.reshape(8, 16, 128)


def polar_messages(place, *arrays):
    high, low = c_table()
    vmem = pl.BlockSpec(memory_space=pltpu.VMEM)
    return pl.pallas_call(
        polar_kernel,
        out_shape=jax.ShapeDtypeStruct((8, 8, 2, 16, 128), BF16),
        in_specs=[pl.BlockSpec(memory_space=pltpu.SMEM)] + [vmem] * 12,
        out_specs=vmem,
        scratch_shapes=[
            pltpu.VMEM((512, 256), F32),
            pltpu.VMEM((1024, 256), BF16),
            pltpu.VMEM((512, 256), BF16),
        ],
        compiler_params=pltpu.CompilerParams(vmem_limit_bytes=LIMIT),
        name="polar",
    )(place, *arrays, high, low)


def finish_kernel(x_ref, a_high_ref, a_low_ref, b_high_ref, b_low_ref, real_ref, imag_ref):
    planes = []
    for block in range(4):
        zb, half = divmod(block, 2)
        x = jnp.concatenate(
            [x_ref[2 * k + zb, :, half].reshape(128, 128) for k in range(4)], axis=0
        )
        planes.append(dot(a_high_ref[...], x) + dot(a_low_ref[...], x))
    for g in range(8):
        z = jnp.concatenate([plane[64 * g : 64 * (g + 1)] for plane in planes], axis=0).T
        z_high = z.astype(BF16)
        z_low = (z - z_high.astype(F32)).astype(BF16)
        out = (
            dot(z_high, b_high_ref[...])
            + dot(z_high, b_low_ref[...])
            + dot(z_low, b_high_ref[...])
        )
        for i in range(4):
            real_ref[:, i, 128 * g : 128 * (g + 1)] = out[32 * i : 32 * (i + 1), :128]
            imag_ref[:, i, 128 * g : 128 * (g + 1)] = out[32 * i : 32 * (i + 1), 128:]


def finish(x):
    vmem = pl.BlockSpec(memory_space=pltpu.VMEM)
    shape = jax.ShapeDtypeStruct((32, 4, 1024), F32)
    return pl.pallas_call(
        finish_kernel,
        out_shape=(shape, shape),
        in_specs=[vmem] * 5,
        out_specs=(vmem, vmem),
        compiler_params=pltpu.CompilerParams(vmem_limit_bytes=LIMIT),
        name="finish",
    )(x, *a_table(), *b_table())


def join_kernel(first_ref, second_ref, out_ref):
    out_ref[:256] = first_ref[:256]
    out_ref[256:] = second_ref[:256]


def join(first, second):
    vmem = pl.BlockSpec(memory_space=pltpu.VMEM)
    return pl.pallas_call(
        join_kernel,
        out_shape=jax.ShapeDtypeStruct((512, 128), BF16),
        in_specs=[vmem, vmem],
        out_specs=vmem,
        compiler_params=pltpu.CompilerParams(vmem_limit_bytes=LIMIT),
        name="join",
    )(first, second)


def fence(x):
    anywhere = pl.BlockSpec(memory_space=pl.ANY)
    return pl.pallas_call(
        lambda in_ref, out_ref: None,
        out_shape=jax.ShapeDtypeStruct(x.shape, x.dtype),
        in_specs=[anywhere],
        out_specs=anywhere,
        input_output_aliases={0: 0},
        compiler_params=pltpu.CompilerParams(vmem_limit_bytes=LIMIT),
        name="fence",
    )(x)


def shift(x, axes, count, by):
    return lax.ppermute(x, axes, [(i, (i + by) % count) for i in range(count)])


def swap(x, axis):
    return lax.ppermute(x, axis, [(0, 1), (1, 0)])


def body(occ, vir, occ_decay, vir_decay):
    row = lax.axis_index(ROW).astype(jnp.int32).reshape(1)
    place = jnp.stack([lax.axis_index(a).astype(jnp.int32) for a in ("c", "z0", "xl", Y)])
    scattered = lax.all_to_all(prepare(row, occ_decay, vir_decay, occ, vir), COL, 0, 0, tiled=True)
    arrived = lax.all_to_all(pack(occ, vir, scattered), ROW, 0, 0, tiled=True)

    near = jnp.concatenate(
        [arrived[:, 48:56].reshape(256, 128), arrived[:, 56:].reshape(256, 128)], axis=0
    )
    near = [near]
    for by in (1, 2, 3):
        near.append(shift(near[0], Y, 4, by))
    up = join(near[0], near[1])
    up = shift(up, ("xh", "xl"), 4, 1)
    down = join(near[2], near[3])
    down = shift(down, ("xh", "xl"), 4, -1)

    def by_group(part, count):
        part = part.reshape(32, count, 8, 128)
        return jnp.transpose(part, (1, 0, 2, 3)).reshape(256 * count, 128)

    own = jnp.concatenate([by_group(arrived[:, :32], 4), by_group(arrived[:, 32:48], 2)], axis=0)
    across = swap(own, "z0")
    beside = swap(own, "c")
    beside = fence(beside)
    opposite = swap(across, "c")
    points = (own, beside, across, opposite)
    messages = polar_messages(place, *points, *near, up, down)

    names = ("xh", "z2", "z1", *COL)
    bits = messages.reshape(2, 2, 2, 2, 2, 2, 32, 128)
    sent = jnp.transpose(bits, (*(names.index(a) for a in LAST), 6, 7)).reshape(64, 32, 128)
    received = lax.all_to_all(sent, LAST, 0, 0, tiled=True).reshape(bits.shape)
    received = jnp.transpose(received, (*(LAST.index(a) for a in names), 6, 7))
    return finish(received.reshape(8, 8, 2, 16, 128))


def solution(mesh):
    fine = Mesh(mesh.devices.reshape((2,) * len(FINE)), FINE)
    return jax.shard_map(
        body,
        mesh=fine,
        in_specs=(P(ROW, COL), P(ROW, COL), P(), P()),
        out_specs=(P(ROW, COL, None), P(ROW, COL, None)),
        check_vma=False,
    )
```

```python
import math

import jax
import jax.numpy as jnp
import numpy as np
from jax import lax
from jax.experimental import pallas as pl
from jax.experimental.pallas import tpu as pltpu
from jax.sharding import Mesh, PartitionSpec as P


NOCC = 1024
NVIR = 512
NGRID = 32768
POLAR_FACTOR = -1.0 / math.sqrt(NOCC * NVIR)
NORMAL = 1.0 / math.sqrt(NGRID)
Z = ("z2", "z1", "z0")
Y = ("y1", "y0")
ROW = ("xh", *Z, "c")
COL = ("xl", *Y)
FINE = ROW + COL
LAST = ("z1", "xl", "y0", "z2", "xh", "y1")
BF16 = jnp.bfloat16
F32 = jnp.float32
LIMIT = 16 * 1024 * 1024


def place_in_last(m, j):
    bits = dict(zip(("xh", "z2", "z1"), ((m >> 2) & 1, (m >> 1) & 1, m & 1)))
    bits.update(zip(COL, ((j >> 2) & 1, (j >> 1) & 1, j & 1)))
    place = 0
    for axis in LAST:
        place = 2 * place + bits[axis]
    return place


def split_table(table):
    high = table.astype(np.float32).astype(jnp.bfloat16)
    low = (table - high.astype(np.float64)).astype(np.float32).astype(jnp.bfloat16)
    return high, low


def rotation(phase):
    cosine, sine = np.cos(phase), np.sin(phase)
    return np.array([[cosine, sine], [-sine, cosine]])


def c_table():
    kc = np.arange(32).reshape(8, 4)
    turn = rotation(2 * np.pi * (kc[..., None] * np.arange(32) % 32) / 32)[:, 0]
    full = np.einsum("pjic,bd->ijpbdc", turn, np.eye(8))
    return split_table(full.reshape(512, 256))


def a_table():
    ka = np.arange(32)
    turn = rotation(2 * np.pi * (ka[:, None] * ka[None, :] % 32) / 32)
    turn = turn.reshape(2, 2, 8, 4, 8, 4)
    full = np.einsum("pqghck,bd->ghpbkcqd", turn, np.eye(8))
    return split_table(full.reshape(512, 512))


def b_table():
    kb = np.arange(32)
    turn = rotation(2 * np.pi * (kb[:, None] * kb[None, :] % 32) / 32) * NORMAL
    turn = turn.reshape(2, 2, 32, 4, 8)
    full = np.einsum("pqkBb,hj->Bhqbpjk", turn, np.eye(4))
    return split_table(full.reshape(256, 256))


def dot(a, b):
    return lax.dot_general(a, b, (((1,), (0,)), ((), ())), preferred_element_type=F32)


def prepare_kernel(place_ref, occ_decay_ref, vir_decay_ref, occ_ref, vir_ref, out_ref):
    row = place_ref[0]

    def column(decay_ref, count):
        index = lax.broadcasted_iota(jnp.int32, (count, 128), 0)
        out = jnp.zeros((count, 128), F32)
        for i in range(count):
            out = jnp.where(index == i, decay_ref[row * count + i], out)
        return out

    def scaled_tiles(ref, decay):
        tiles = [ref[:, 128 * t : 128 * (t + 1)].astype(F32) * decay for t in range(8)]
        return [
            [
                jnp.concatenate(
                    [tiles[4 * t + u][:, 32 * kind : 32 * (kind + 1)] for u in range(4)], axis=1
                )
                for kind in range(4)
            ]
            for t in range(2)
        ]

    occ = scaled_tiles(occ_ref, column(occ_decay_ref, 32))
    vir = scaled_tiles(vir_ref, column(vir_decay_ref, 16))
    for y1 in range(2):
        for t in range(2):
            for kind in range(4):
                piece = jnp.concatenate(
                    [
                        occ[t][kind][8 * y1 : 8 * (y1 + 1)],
                        occ[t][kind][8 * (2 + y1) : 8 * (3 + y1)],
                        vir[t][kind][8 * y1 : 8 * (y1 + 1)],
                    ],
                    axis=0,
                ).astype(BF16)
                for xl in range(2):
                    out_ref[4 * xl + 2 * y1 + t, kind] = piece


def prepare(place, occ_decay, vir_decay, occ, vir):
    smem = pl.BlockSpec(memory_space=pltpu.SMEM)
    return pl.pallas_call(
        prepare_kernel,
        grid=(1,),
        out_shape=jax.ShapeDtypeStruct((8, 4, 24, 128), BF16),
        in_specs=[
            smem,
            smem,
            smem,
            pl.BlockSpec((32, 1024), lambda i: (0, 0)),
            pl.BlockSpec((16, 1024), lambda i: (0, 0)),
        ],
        out_specs=pl.BlockSpec((8, 4, 24, 128), lambda i: (0, 0, 0, 0)),
        name="prepare",
    )(place, occ_decay, vir_decay, occ, vir)


def pack_kernel(occ_ref, vir_ref, rows_ref, out_ref):
    for p in range(32):
        out_ref[p, 0:32, :] = occ_ref[:, 128 * p : 128 * (p + 1)]
        out_ref[p, 32:48, :] = vir_ref[:, 128 * p : 128 * (p + 1)]
        out_ref[p, 48:72, :] = rows_ref[0, p % 4]


def pack(occ, vir, rows):
    vmem = pl.BlockSpec(memory_space=pltpu.VMEM)
    return pl.pallas_call(
        pack_kernel,
        out_shape=jax.ShapeDtypeStruct((32, 72, 128), BF16),
        in_specs=[vmem] * 3,
        out_specs=vmem,
        compiler_params=pltpu.CompilerParams(vmem_limit_bytes=LIMIT),
        name="pack",
    )(occ, vir, rows)


def polar_kernel(core_ref, z0_ref, y_ref, *refs):
    points, near, (high_ref, low_ref) = refs[:4], refs[4:8], refs[8:10]
    out_ref, polar_ref, occ_ref, vir_ref = refs[-4:]
    core, z0, y = core_ref[0], z0_ref[0], y_ref[0]
    for step in range(4):
        chunk = lax.rem(y + 4 - step, 4)
        y1, y0 = lax.div(chunk, 2), lax.rem(chunk, 2)
        lanes = pl.ds(pl.multiple_of(128 * y0, 128), 128)

        def rows(group):
            return pl.ds(pl.multiple_of(256 * group, 256), 256)

        occ_ref[rows(y1), lanes] = near[step][:256]
        occ_ref[rows(2 + y1), lanes] = near[step][256:512]
        vir_ref[rows(y1), lanes] = near[step][512:]
    for k, ref in enumerate(points):
        place = 2 * (z0 if k < 2 else 1 - z0) + (core if k % 2 == 0 else 1 - core)
        green_occ = dot(ref[:1024].T, occ_ref[...])
        green_vir = dot(ref[1024:].T, vir_ref[...])
        polar_ref[pl.ds(pl.multiple_of(128 * place, 128), 128), :] = (
            green_occ * green_vir * POLAR_FACTOR
        )
    for half in range(2):
        polar = polar_ref[256 * half : 256 * (half + 1), :]
        polar_high = polar.astype(BF16)
        polar_low = (polar - polar_high.astype(F32)).astype(BF16)
        spectrum = (
            dot(high_ref[...], polar_high)
            + dot(high_ref[...], polar_low)
            + dot(low_ref[...], polar_high)
        )
        for m in range(8):
            pieces = [spectrum[128 * i : 128 * (i + 1), 32 * m : 32 * (m + 1)] for i in range(4)]
            message = jnp.concatenate(pieces, axis=1).astype(BF16)
            for j in range(8):
                out_ref[place_in_last(m, j), half] = message[16 * j : 16 * (j + 1)]


def polar_messages(*arrays):
    vmem = pl.BlockSpec(memory_space=pltpu.VMEM)
    return pl.pallas_call(
        polar_kernel,
        out_shape=jax.ShapeDtypeStruct((64, 2, 16, 128), BF16),
        in_specs=[pl.BlockSpec(memory_space=pltpu.SMEM)] * 3 + [vmem] * 10,
        out_specs=vmem,
        scratch_shapes=[
            pltpu.VMEM((512, 256), F32),
            pltpu.VMEM((1024, 256), BF16),
            pltpu.VMEM((512, 256), BF16),
        ],
        compiler_params=pltpu.CompilerParams(vmem_limit_bytes=LIMIT),
        name="polar",
    )(*arrays)


def finish_kernel(x_ref, a_high_ref, a_low_ref, b_high_ref, b_low_ref, *refs):
    outs, parts, sems = refs[:2], refs[2:4], refs[4]
    planes = []
    for block in range(4):
        zb, half = divmod(block, 2)
        x = jnp.concatenate(
            [x_ref[place_in_last(2 * k + zb, j), half] for k in range(4) for j in range(8)], axis=0
        )
        planes.append(dot(a_high_ref[...], x) + dot(a_low_ref[...], x))
    copies = []
    for g in range(8):
        z = jnp.concatenate([plane[64 * g : 64 * (g + 1)] for plane in planes], axis=0).T
        z_high = z.astype(BF16)
        z_low = (z - z_high.astype(F32)).astype(BF16)
        out = (
            dot(z_high, b_high_ref[...])
            + dot(z_high, b_low_ref[...])
            + dot(z_low, b_high_ref[...])
        )
        for which in range(2):
            for i in range(4):
                parts[which][:, i, 128 * g : 128 * (g + 1)] = out[
                    32 * i : 32 * (i + 1), 128 * which : 128 * (which + 1)
                ]
            if g % 2 == 1:
                lanes = pl.ds(128 * (g - 1), 256)
                copy = pltpu.make_async_copy(
                    parts[which].at[:, :, lanes], outs[which].at[:, :, lanes], sems.at[which, g // 2]
                )
                copy.start()
                copies.append(copy)
    for copy in copies:
        copy.wait()


def finish(x, *tables):
    vmem = pl.BlockSpec(memory_space=pltpu.VMEM)
    hbm = pl.BlockSpec(memory_space=pl.ANY)
    shape = jax.ShapeDtypeStruct((32, 4, 1024), F32)
    return pl.pallas_call(
        finish_kernel,
        out_shape=(shape, shape),
        in_specs=[vmem] * 5,
        out_specs=(hbm, hbm),
        scratch_shapes=[
            pltpu.VMEM((32, 4, 1024), F32),
            pltpu.VMEM((32, 4, 1024), F32),
            pltpu.SemaphoreType.DMA((2, 4)),
        ],
        compiler_params=pltpu.CompilerParams(vmem_limit_bytes=LIMIT),
        name="finish",
    )(x, *tables)


def carry_kernel(*refs):
    count = len(refs) // 2
    for in_ref, out_ref in zip(refs[:count], refs[count:]):
        out_ref[...] = in_ref[...]


def carry(*arrays):
    vmem = pl.BlockSpec(memory_space=pltpu.VMEM)
    return pl.pallas_call(
        carry_kernel,
        out_shape=[jax.ShapeDtypeStruct(a.shape, a.dtype) for a in arrays],
        in_specs=[vmem] * len(arrays),
        out_specs=[vmem] * len(arrays),
        compiler_params=pltpu.CompilerParams(vmem_limit_bytes=LIMIT),
        name="carry",
    )(*arrays)


def fence(x):
    anywhere = pl.BlockSpec(memory_space=pl.ANY)
    return pl.pallas_call(
        lambda in_ref, out_ref: None,
        out_shape=jax.ShapeDtypeStruct(x.shape, x.dtype),
        in_specs=[anywhere],
        out_specs=anywhere,
        input_output_aliases={0: 0},
        compiler_params=pltpu.CompilerParams(vmem_limit_bytes=LIMIT),
        name="fence",
    )(x)


def shift(x, axes, count, by):
    return lax.ppermute(x, axes, [(i, (i + by) % count) for i in range(count)])


def swap(x, axis):
    return lax.ppermute(x, axis, [(0, 1), (1, 0)])


def body(occ, vir, occ_decay, vir_decay):
    row = lax.axis_index(ROW).astype(jnp.int32).reshape(1)
    place = [lax.axis_index(a).astype(jnp.int32).reshape(1) for a in ("c", "z0", Y)]
    scattered = lax.all_to_all(prepare(row, occ_decay, vir_decay, occ, vir), COL, 0, 0, tiled=True)
    arrived = lax.all_to_all(pack(occ, vir, scattered), ROW, 0, 0, tiled=True)

    def by_group(part, count):
        part = part.reshape(32, count, 8, 128)
        return jnp.transpose(part, (1, 0, 2, 3)).reshape(256 * count, 128)

    near = jnp.concatenate([by_group(arrived[:, 48:64], 2), by_group(arrived[:, 64:], 1)], axis=0)
    near = [near]
    for by in (1, 2, 3):
        near.append(shift(near[0], Y, 4, by))
    own = jnp.concatenate([by_group(arrived[:, :32], 4), by_group(arrived[:, 32:48], 2)], axis=0)
    across = swap(own, "z0")
    beside = swap(own, "c")
    beside = fence(beside)
    opposite = swap(across, "c")
    points = (own, beside, across, opposite)
    messages = polar_messages(*place, *points, *near, *c_table())

    received = lax.all_to_all(messages, LAST, 0, 0, tiled=True)
    tables = carry(*a_table(), *b_table())
    return finish(received, *tables)


def solution(mesh):
    fine = Mesh(mesh.devices.reshape((2,) * len(FINE)), FINE)
    return jax.shard_map(
        body,
        mesh=fine,
        in_specs=(P(ROW, COL), P(ROW, COL), P(), P()),
        out_specs=(P(ROW, COL, None), P(ROW, COL, None)),
        check_vma=False,
    )
```

```python
import math

import jax
import jax.numpy as jnp
import numpy as np
from jax import lax
from jax.experimental import pallas as pl
from jax.experimental.pallas import tpu as pltpu
from jax.sharding import Mesh, PartitionSpec as P


NOCC = 1024
NVIR = 512
NGRID = 32768
POLAR_FACTOR = -1.0 / math.sqrt(NOCC * NVIR)
NORMAL = 1.0 / math.sqrt(NGRID)
Z = ("z2", "z1", "z0")
Y = ("y1", "y0")
ROW = ("xh", *Z, "c")
COL = ("xl", *Y)
FINE = ROW + COL
LAST = ("z1", "xl", "y0", "z2", "xh", "y1")
BF16 = jnp.bfloat16
F32 = jnp.float32
LIMIT = 16 * 1024 * 1024


def place_in_last(m, j):
    bits = dict(zip(("xh", "z2", "z1"), ((m >> 2) & 1, (m >> 1) & 1, m & 1)))
    bits.update(zip(COL, ((j >> 2) & 1, (j >> 1) & 1, j & 1)))
    place = 0
    for axis in LAST:
        place = 2 * place + bits[axis]
    return place


def split_table(table):
    high = table.astype(np.float32).astype(jnp.bfloat16)
    low = (table - high.astype(np.float64)).astype(np.float32).astype(jnp.bfloat16)
    return high, low


def rotation(phase):
    cosine, sine = np.cos(phase), np.sin(phase)
    return np.array([[cosine, sine], [-sine, cosine]])


def c_table():
    kc = np.arange(32).reshape(8, 4)
    turn = rotation(2 * np.pi * (kc[..., None] * np.arange(32) % 32) / 32)[:, 0]
    full = np.einsum("pjic,bd->ijpbdc", turn, np.eye(8))
    return split_table(full.reshape(512, 256))


def a_table():
    ka = np.arange(32)
    turn = rotation(2 * np.pi * (ka[:, None] * ka[None, :] % 32) / 32)
    turn = turn.reshape(2, 2, 8, 4, 8, 4)
    full = np.einsum("pqghck,bd->ghpbkcqd", turn, np.eye(8))
    return split_table(full.reshape(512, 512))


def b_table():
    kb = np.arange(32)
    turn = rotation(2 * np.pi * (kb[:, None] * kb[None, :] % 32) / 32) * NORMAL
    turn = turn.reshape(2, 2, 32, 4, 8)
    full = np.einsum("pqkBb,hj->Bhqbpjk", turn, np.eye(4))
    return split_table(full.reshape(256, 256))


def dot(a, b):
    return lax.dot_general(a, b, (((1,), (0,)), ((), ())), preferred_element_type=F32)


def prepare_kernel(row_ref, col_ref, *refs):
    @pl.when(col_ref[0] == 0)
    def _():
        prepare_rows(row_ref[0], *refs)


def prepare_rows(
    row, occ_decay_ref, vir_decay_ref, occ_hbm, vir_hbm, out_hbm, occ_ref, vir_ref, out_ref, sems
):
    copies = [
        pltpu.make_async_copy(occ_hbm.at[:, :1024], occ_ref, sems.at[0]),
        pltpu.make_async_copy(vir_hbm.at[:, :1024], vir_ref, sems.at[1]),
    ]
    for copy in copies:
        copy.start()
    for copy in copies:
        copy.wait()

    def column(decay_ref, count):
        index = lax.broadcasted_iota(jnp.int32, (count, 128), 0)
        out = jnp.zeros((count, 128), F32)
        for i in range(count):
            out = jnp.where(index == i, decay_ref[row * count + i], out)
        return out

    def scaled_tiles(ref, decay):
        tiles = [ref[:, 128 * t : 128 * (t + 1)].astype(F32) * decay for t in range(8)]
        return [
            [
                jnp.concatenate(
                    [tiles[4 * t + u][:, 32 * kind : 32 * (kind + 1)] for u in range(4)], axis=1
                )
                for kind in range(4)
            ]
            for t in range(2)
        ]

    occ = scaled_tiles(occ_ref, column(occ_decay_ref, 32))
    vir = scaled_tiles(vir_ref, column(vir_decay_ref, 16))
    for y1 in range(2):
        for t in range(2):
            for kind in range(4):
                piece = jnp.concatenate(
                    [
                        occ[t][kind][8 * y1 : 8 * (y1 + 1)],
                        occ[t][kind][8 * (2 + y1) : 8 * (3 + y1)],
                        vir[t][kind][8 * y1 : 8 * (y1 + 1)],
                    ],
                    axis=0,
                ).astype(BF16)
                for xl in range(2):
                    out_ref[4 * xl + 2 * y1 + t, kind] = piece
    result = pltpu.make_async_copy(out_ref, out_hbm, sems.at[2])
    result.start()
    result.wait()


def prepare(row, col, occ_decay, vir_decay, occ, vir):
    smem = pl.BlockSpec(memory_space=pltpu.SMEM)
    hbm = pl.BlockSpec(memory_space=pl.ANY)
    return pl.pallas_call(
        prepare_kernel,
        out_shape=jax.ShapeDtypeStruct((8, 4, 24, 128), BF16),
        in_specs=[smem] * 4 + [hbm] * 2,
        out_specs=hbm,
        scratch_shapes=[
            pltpu.VMEM((32, 1024), BF16),
            pltpu.VMEM((16, 1024), BF16),
            pltpu.VMEM((8, 4, 24, 128), BF16),
            pltpu.SemaphoreType.DMA((3,)),
        ],
        name="prepare",
    )(row, col, occ_decay, vir_decay, occ, vir)


def pack_kernel(occ_ref, vir_ref, rows_ref, out_ref):
    for p in range(32):
        out_ref[p, 0:32, :] = occ_ref[:, 128 * p : 128 * (p + 1)]
        out_ref[p, 32:48, :] = vir_ref[:, 128 * p : 128 * (p + 1)]
        out_ref[p, 48:72, :] = rows_ref[0, p % 4]


def pack(occ, vir, rows):
    vmem = pl.BlockSpec(memory_space=pltpu.VMEM)
    return pl.pallas_call(
        pack_kernel,
        out_shape=jax.ShapeDtypeStruct((32, 72, 128), BF16),
        in_specs=[vmem] * 3,
        out_specs=vmem,
        compiler_params=pltpu.CompilerParams(vmem_limit_bytes=LIMIT),
        name="pack",
    )(occ, vir, rows)


def polar_kernel(core_ref, z0_ref, y_ref, *refs):
    points, near, (high_ref, low_ref) = refs[:4], refs[4:8], refs[8:10]
    out_ref, polar_ref, occ_ref, vir_ref = refs[-4:]
    core, z0, y = core_ref[0], z0_ref[0], y_ref[0]
    for step in range(4):
        chunk = lax.rem(y + 4 - step, 4)
        y1, y0 = lax.div(chunk, 2), lax.rem(chunk, 2)
        lanes = pl.ds(pl.multiple_of(128 * y0, 128), 128)

        def rows(group):
            return pl.ds(pl.multiple_of(256 * group, 256), 256)

        occ_ref[rows(y1), lanes] = near[step][:256]
        occ_ref[rows(2 + y1), lanes] = near[step][256:512]
        vir_ref[rows(y1), lanes] = near[step][512:]
    occ = jnp.concatenate([ref[:1024].T for ref in points], axis=0)
    vir = jnp.concatenate([ref[1024:].T for ref in points], axis=0)
    product = dot(occ, occ_ref[...]) * dot(vir, vir_ref[...]) * POLAR_FACTOR
    for k in range(4):
        place = 2 * (z0 if k < 2 else 1 - z0) + (core if k % 2 == 0 else 1 - core)
        polar_ref[pl.ds(pl.multiple_of(128 * place, 128), 128), :] = product[
            128 * k : 128 * (k + 1)
        ]
    for half in range(2):
        polar = polar_ref[256 * half : 256 * (half + 1), :]
        polar_high = polar.astype(BF16)
        polar_low = (polar - polar_high.astype(F32)).astype(BF16)
        spectrum = (
            dot(high_ref[...], polar_high)
            + dot(high_ref[...], polar_low)
            + dot(low_ref[...], polar_high)
        )
        for m in range(8):
            pieces = [spectrum[128 * i : 128 * (i + 1), 32 * m : 32 * (m + 1)] for i in range(4)]
            message = jnp.concatenate(pieces, axis=1).astype(BF16)
            for j in range(8):
                out_ref[place_in_last(m, j), half] = message[16 * j : 16 * (j + 1)]


def polar_messages(*arrays):
    vmem = pl.BlockSpec(memory_space=pltpu.VMEM)
    return pl.pallas_call(
        polar_kernel,
        out_shape=jax.ShapeDtypeStruct((64, 2, 16, 128), BF16),
        in_specs=[pl.BlockSpec(memory_space=pltpu.SMEM)] * 3 + [vmem] * 10,
        out_specs=vmem,
        scratch_shapes=[
            pltpu.VMEM((512, 256), F32),
            pltpu.VMEM((1024, 256), BF16),
            pltpu.VMEM((512, 256), BF16),
        ],
        compiler_params=pltpu.CompilerParams(vmem_limit_bytes=LIMIT),
        name="polar",
    )(*arrays)


def finish_kernel(x_ref, a_high_ref, a_low_ref, b_high_ref, b_low_ref, *refs):
    outs, parts, sems = refs[:2], refs[2:4], refs[4]
    x = jnp.concatenate(
        [
            jnp.concatenate(
                [x_ref[place_in_last(2 * k + block // 2, j), block % 2] for k in range(4) for j in range(8)],
                axis=0,
            )
            for block in range(4)
        ],
        axis=1,
    )
    planes = dot(a_high_ref[...], x) + dot(a_low_ref[...], x)
    copies = []
    for part in range(4):
        z = jnp.concatenate(
            [
                jnp.concatenate(
                    [
                        planes[64 * g : 64 * (g + 1), 128 * block : 128 * (block + 1)]
                        for block in range(4)
                    ],
                    axis=0,
                ).T
                for g in (2 * part, 2 * part + 1)
            ],
            axis=0,
        )
        z_high = z.astype(BF16)
        z_low = (z - z_high.astype(F32)).astype(BF16)
        out = (
            dot(z_high, b_high_ref[...])
            + dot(z_high, b_low_ref[...])
            + dot(z_low, b_high_ref[...])
        )
        for which in range(2):
            for g in range(2):
                for i in range(4):
                    rows = 128 * g + 32 * i
                    parts[which][:, i, 128 * (2 * part + g) : 128 * (2 * part + g + 1)] = out[
                        rows : rows + 32, 128 * which : 128 * (which + 1)
                    ]
            lanes = pl.ds(256 * part, 256)
            copy = pltpu.make_async_copy(
                parts[which].at[:, :, lanes], outs[which].at[:, :, lanes], sems.at[which, part]
            )
            copy.start()
            copies.append(copy)
    for copy in copies:
        copy.wait()


def finish(x, *tables):
    vmem = pl.BlockSpec(memory_space=pltpu.VMEM)
    hbm = pl.BlockSpec(memory_space=pl.ANY)
    shape = jax.ShapeDtypeStruct((32, 4, 1024), F32)
    return pl.pallas_call(
        finish_kernel,
        out_shape=(shape, shape),
        in_specs=[vmem] * 5,
        out_specs=(hbm, hbm),
        scratch_shapes=[
            pltpu.VMEM((32, 4, 1024), F32),
            pltpu.VMEM((32, 4, 1024), F32),
            pltpu.SemaphoreType.DMA((2, 4)),
        ],
        compiler_params=pltpu.CompilerParams(vmem_limit_bytes=LIMIT),
        name="finish",
    )(x, *tables)


def carry_kernel(*refs):
    count = len(refs) // 2
    for in_ref, out_ref in zip(refs[:count], refs[count:]):
        out_ref[...] = in_ref[...]


def carry(*arrays):
    vmem = pl.BlockSpec(memory_space=pltpu.VMEM)
    return pl.pallas_call(
        carry_kernel,
        out_shape=[jax.ShapeDtypeStruct(a.shape, a.dtype) for a in arrays],
        in_specs=[vmem] * len(arrays),
        out_specs=[vmem] * len(arrays),
        compiler_params=pltpu.CompilerParams(vmem_limit_bytes=LIMIT),
        name="carry",
    )(*arrays)


def fence(x):
    anywhere = pl.BlockSpec(memory_space=pl.ANY)
    return pl.pallas_call(
        lambda in_ref, out_ref: None,
        out_shape=jax.ShapeDtypeStruct(x.shape, x.dtype),
        in_specs=[anywhere],
        out_specs=anywhere,
        input_output_aliases={0: 0},
        compiler_params=pltpu.CompilerParams(vmem_limit_bytes=LIMIT),
        name="fence",
    )(x)


def shift(x, axes, count, by):
    return lax.ppermute(x, axes, [(i, (i + by) % count) for i in range(count)])


def swap(x, axis):
    return lax.ppermute(x, axis, [(0, 1), (1, 0)])


def body(occ, vir, occ_decay, vir_decay):
    row = lax.axis_index(ROW).astype(jnp.int32).reshape(1)
    col = lax.axis_index(COL).astype(jnp.int32).reshape(1)
    place = [lax.axis_index(a).astype(jnp.int32).reshape(1) for a in ("c", "z0", Y)]
    scattered = lax.all_to_all(prepare(row, col, occ_decay, vir_decay, occ, vir), COL, 0, 0, tiled=True)
    arrived = lax.all_to_all(pack(occ, vir, scattered), ROW, 0, 0, tiled=True)

    def by_group(part, count):
        part = part.reshape(32, count, 8, 128)
        return jnp.transpose(part, (1, 0, 2, 3)).reshape(256 * count, 128)

    near = jnp.concatenate([by_group(arrived[:, 48:64], 2), by_group(arrived[:, 64:], 1)], axis=0)
    near = [near]
    for by in (1, 2, 3):
        near.append(shift(near[0], Y, 4, by))
    own = jnp.concatenate([by_group(arrived[:, :32], 4), by_group(arrived[:, 32:48], 2)], axis=0)
    across = swap(own, "z0")
    beside = swap(own, "c")
    beside = fence(beside)
    opposite = swap(across, "c")
    points = (own, beside, across, opposite)
    messages = polar_messages(*place, *points, *near, *c_table())

    received = lax.all_to_all(messages, LAST, 0, 0, tiled=True)
    tables = carry(*a_table(), *b_table())
    return finish(received, *tables)


def solution(mesh):
    fine = Mesh(mesh.devices.reshape((2,) * len(FINE)), FINE)
    return jax.shard_map(
        body,
        mesh=fine,
        in_specs=(P(ROW, COL), P(ROW, COL), P(), P()),
        out_specs=(P(ROW, COL, None), P(ROW, COL, None)),
        check_vma=False,
    )
```

```python
import math

import jax
import jax.numpy as jnp
import numpy as np
from jax import lax
from jax.experimental import pallas as pl
from jax.experimental.pallas import tpu as pltpu
from jax.sharding import Mesh, PartitionSpec as P


NOCC = 1024
NVIR = 512
NGRID = 32768
POLAR_FACTOR = -1.0 / math.sqrt(NOCC * NVIR)
NORMAL = 1.0 / math.sqrt(NGRID)
Z = ("z2", "z1", "z0")
Y = ("y1", "y0")
ROW = ("xh", *Z, "c")
COL = ("xl", *Y)
FINE = ROW + COL
LAST = ("z1", "xl", "y0", "z2", "xh", "y1")
BF16 = jnp.bfloat16
F32 = jnp.float32
LIMIT = 16 * 1024 * 1024


def place_in_last(m, j):
    bits = dict(zip(("xh", "z2", "z1"), ((m >> 2) & 1, (m >> 1) & 1, m & 1)))
    bits.update(zip(COL, ((j >> 2) & 1, (j >> 1) & 1, j & 1)))
    place = 0
    for axis in LAST:
        place = 2 * place + bits[axis]
    return place


def split_table(table):
    high = table.astype(np.float32).astype(jnp.bfloat16)
    low = (table - high.astype(np.float64)).astype(np.float32).astype(jnp.bfloat16)
    return high, low


def rotation(phase):
    cosine, sine = np.cos(phase), np.sin(phase)
    return np.array([[cosine, sine], [-sine, cosine]])


def c_table():
    kc = np.arange(32).reshape(8, 4)
    turn = rotation(2 * np.pi * (kc[..., None] * np.arange(32) % 32) / 32)[:, 0]
    full = np.einsum("pjic,bd->ijpbdc", turn, np.eye(8))
    return split_table(full.reshape(512, 256))


def a_table():
    ka = np.arange(32)
    turn = rotation(2 * np.pi * (ka[:, None] * ka[None, :] % 32) / 32)
    turn = turn.reshape(2, 2, 8, 4, 8, 4)
    full = np.einsum("pqghck,bd->ghpbkcqd", turn, np.eye(8))
    return split_table(full.reshape(512, 512))


def b_table():
    kb = np.arange(32)
    turn = rotation(2 * np.pi * (kb[:, None] * kb[None, :] % 32) / 32) * NORMAL
    turn = turn.reshape(2, 2, 32, 4, 8)
    full = np.einsum("pqkBb,hj->Bhqbpjk", turn, np.eye(4))
    return split_table(full.reshape(256, 256))


def dot(a, b):
    return lax.dot_general(a, b, (((1,), (0,)), ((), ())), preferred_element_type=F32)


def prepare_kernel(row_ref, col_ref, *refs):
    @pl.when(col_ref[0] == 0)
    def _():
        prepare_rows(row_ref[0], *refs)


def prepare_rows(
    row, occ_decay_ref, vir_decay_ref, occ_hbm, vir_hbm, out_hbm, occ_ref, vir_ref, out_ref, sems
):
    copies = [
        pltpu.make_async_copy(occ_hbm.at[:, :1024], occ_ref, sems.at[0]),
        pltpu.make_async_copy(vir_hbm.at[:, :1024], vir_ref, sems.at[1]),
    ]
    for copy in copies:
        copy.start()
    for copy in copies:
        copy.wait()

    def column(decay_ref, count):
        index = lax.broadcasted_iota(jnp.int32, (count, 128), 0)
        out = jnp.zeros((count, 128), F32)
        for i in range(count):
            out = jnp.where(index == i, decay_ref[row * count + i], out)
        return out

    def scaled_tiles(ref, decay):
        tiles = [ref[:, 128 * t : 128 * (t + 1)].astype(F32) * decay for t in range(8)]
        return [
            [
                jnp.concatenate(
                    [tiles[4 * t + u][:, 32 * kind : 32 * (kind + 1)] for u in range(4)], axis=1
                )
                for kind in range(4)
            ]
            for t in range(2)
        ]

    occ = scaled_tiles(occ_ref, column(occ_decay_ref, 32))
    vir = scaled_tiles(vir_ref, column(vir_decay_ref, 16))
    for xl in range(2):
        for y1 in range(2):
            for t in range(2):
                for kind in range(4):
                    group = 2 * xl + y1
                    piece = jnp.concatenate(
                        [
                            occ[t][kind][8 * group : 8 * (group + 1)],
                            vir[t][kind][8 * y1 : 8 * (y1 + 1)],
                        ],
                        axis=0,
                    )
                    peer = 8 * (kind % 2) + 4 * xl + 2 * y1 + t
                    out_ref[peer, kind // 2] = piece.astype(BF16)
    result = pltpu.make_async_copy(out_ref, out_hbm, sems.at[2])
    result.start()
    result.wait()


def prepare(row, col, occ_decay, vir_decay, occ, vir):
    smem = pl.BlockSpec(memory_space=pltpu.SMEM)
    hbm = pl.BlockSpec(memory_space=pl.ANY)
    return pl.pallas_call(
        prepare_kernel,
        out_shape=jax.ShapeDtypeStruct((16, 2, 16, 128), BF16),
        in_specs=[smem] * 4 + [hbm] * 2,
        out_specs=hbm,
        scratch_shapes=[
            pltpu.VMEM((32, 1024), BF16),
            pltpu.VMEM((16, 1024), BF16),
            pltpu.VMEM((16, 2, 16, 128), BF16),
            pltpu.SemaphoreType.DMA((3,)),
        ],
        name="prepare",
    )(row, col, occ_decay, vir_decay, occ, vir)


def divide_kernel(core_ref, occ_ref, vir_ref, kept_ref, sent_ref):
    core = core_ref[0]
    for out_ref, which in ((kept_ref, core), (sent_ref, 1 - core)):
        for p in range(16):
            lanes = pl.ds(pl.multiple_of(128 * (2 * p + which), 128), 128)
            out_ref[p, :32, :] = occ_ref[:, lanes]
            out_ref[p, 32:, :] = vir_ref[:, lanes]


def divide(core, occ, vir):
    vmem = pl.BlockSpec(memory_space=pltpu.VMEM)
    shape = jax.ShapeDtypeStruct((16, 48, 128), BF16)
    return pl.pallas_call(
        divide_kernel,
        out_shape=(shape, shape),
        in_specs=[pl.BlockSpec(memory_space=pltpu.SMEM), vmem, vmem],
        out_specs=(vmem, vmem),
        compiler_params=pltpu.CompilerParams(vmem_limit_bytes=LIMIT),
        name="divide",
    )(core, occ, vir)


def pack_kernel(core_ref, kept_ref, other_ref, rows_ref, out_ref):
    core = core_ref[0]
    out_ref[:, pl.ds(pl.multiple_of(48 * core, 16), 48), :] = kept_ref[...]
    out_ref[:, pl.ds(pl.multiple_of(48 * (1 - core), 16), 48), :] = other_ref[...]
    for p in range(16):
        out_ref[p, 96:112, :] = rows_ref[0, p % 2]
        out_ref[p, 112:128, :] = rows_ref[8, p % 2]


def pack(core, kept, other, rows):
    vmem = pl.BlockSpec(memory_space=pltpu.VMEM)
    return pl.pallas_call(
        pack_kernel,
        out_shape=jax.ShapeDtypeStruct((16, 128, 128), BF16),
        in_specs=[pl.BlockSpec(memory_space=pltpu.SMEM)] + [vmem] * 3,
        out_specs=vmem,
        compiler_params=pltpu.CompilerParams(vmem_limit_bytes=LIMIT),
        name="pack",
    )(core, kept, other, rows)


def polar_kernel(core_ref, z0_ref, xl_ref, y_ref, *refs):
    points, near, far, (high_ref, low_ref) = refs[:4], refs[4:8], refs[8:10], refs[10:12]
    out_ref, polar_ref, occ_ref, vir_ref = refs[-4:]
    core, z0, xl, y = core_ref[0], z0_ref[0], xl_ref[0], y_ref[0]
    for step in range(4):
        chunk = lax.rem(y + 4 - step, 4)
        y1, y0 = lax.div(chunk, 2), lax.rem(chunk, 2)
        lanes = pl.ds(pl.multiple_of(128 * y0, 128), 128)

        def rows(group):
            return pl.ds(pl.multiple_of(256 * group, 256), 256)

        occ_ref[rows(2 * xl + y1), lanes] = near[step][:256]
        occ_ref[rows(2 * (1 - xl) + y1), lanes] = far[step // 2][
            256 * (step % 2) : 256 * (step % 2 + 1)
        ]
        vir_ref[rows(y1), lanes] = near[step][256:]
    occ = jnp.concatenate([ref[:1024].T for ref in points], axis=0)
    vir = jnp.concatenate([ref[1024:].T for ref in points], axis=0)
    product = dot(occ, occ_ref[...]) * dot(vir, vir_ref[...]) * POLAR_FACTOR
    for k in range(4):
        place = 2 * (z0 if k < 2 else 1 - z0) + (core if k % 2 == 0 else 1 - core)
        polar_ref[pl.ds(pl.multiple_of(128 * place, 128), 128), :] = product[
            128 * k : 128 * (k + 1)
        ]
    for half in range(2):
        polar = polar_ref[256 * half : 256 * (half + 1), :]
        polar_high = polar.astype(BF16)
        polar_low = (polar - polar_high.astype(F32)).astype(BF16)
        spectrum = (
            dot(high_ref[...], polar_high)
            + dot(high_ref[...], polar_low)
            + dot(low_ref[...], polar_high)
        )
        for m in range(8):
            pieces = [spectrum[128 * i : 128 * (i + 1), 32 * m : 32 * (m + 1)] for i in range(4)]
            message = jnp.concatenate(pieces, axis=1).astype(BF16)
            for j in range(8):
                out_ref[place_in_last(m, j), half] = message[16 * j : 16 * (j + 1)]


def polar_messages(*arrays):
    vmem = pl.BlockSpec(memory_space=pltpu.VMEM)
    return pl.pallas_call(
        polar_kernel,
        out_shape=jax.ShapeDtypeStruct((64, 2, 16, 128), BF16),
        in_specs=[pl.BlockSpec(memory_space=pltpu.SMEM)] * 4 + [vmem] * 12,
        out_specs=vmem,
        scratch_shapes=[
            pltpu.VMEM((512, 256), F32),
            pltpu.VMEM((1024, 256), BF16),
            pltpu.VMEM((512, 256), BF16),
        ],
        compiler_params=pltpu.CompilerParams(vmem_limit_bytes=LIMIT),
        name="polar",
    )(*arrays)


def finish_kernel(x_ref, a_high_ref, a_low_ref, b_high_ref, b_low_ref, *refs):
    outs, parts, sems = refs[:2], refs[2:4], refs[4]
    x = jnp.concatenate(
        [
            jnp.concatenate(
                [x_ref[place_in_last(2 * k + block // 2, j), block % 2] for k in range(4) for j in range(8)],
                axis=0,
            )
            for block in range(4)
        ],
        axis=1,
    )
    planes = dot(a_high_ref[...], x) + dot(a_low_ref[...], x)
    copies = []
    for part in range(4):
        z = jnp.concatenate(
            [
                jnp.concatenate(
                    [
                        planes[64 * g : 64 * (g + 1), 128 * block : 128 * (block + 1)]
                        for block in range(4)
                    ],
                    axis=0,
                ).T
                for g in (2 * part, 2 * part + 1)
            ],
            axis=0,
        )
        z_high = z.astype(BF16)
        z_low = (z - z_high.astype(F32)).astype(BF16)
        out = (
            dot(z_high, b_high_ref[...])
            + dot(z_high, b_low_ref[...])
            + dot(z_low, b_high_ref[...])
        )
        for which in range(2):
            for g in range(2):
                for i in range(4):
                    rows = 128 * g + 32 * i
                    parts[which][:, i, 128 * (2 * part + g) : 128 * (2 * part + g + 1)] = out[
                        rows : rows + 32, 128 * which : 128 * (which + 1)
                    ]
            lanes = pl.ds(256 * part, 256)
            copy = pltpu.make_async_copy(
                parts[which].at[:, :, lanes], outs[which].at[:, :, lanes], sems.at[which, part]
            )
            copy.start()
            copies.append(copy)
    for copy in copies:
        copy.wait()


def finish(x, *tables):
    vmem = pl.BlockSpec(memory_space=pltpu.VMEM)
    hbm = pl.BlockSpec(memory_space=pl.ANY)
    shape = jax.ShapeDtypeStruct((32, 4, 1024), F32)
    return pl.pallas_call(
        finish_kernel,
        out_shape=(shape, shape),
        in_specs=[vmem] * 5,
        out_specs=(hbm, hbm),
        scratch_shapes=[
            pltpu.VMEM((32, 4, 1024), F32),
            pltpu.VMEM((32, 4, 1024), F32),
            pltpu.SemaphoreType.DMA((2, 4)),
        ],
        compiler_params=pltpu.CompilerParams(vmem_limit_bytes=LIMIT),
        name="finish",
    )(x, *tables)


def join_kernel(first_ref, second_ref, out_ref):
    out_ref[:256] = first_ref[:256]
    out_ref[256:] = second_ref[:256]


def join(first, second):
    vmem = pl.BlockSpec(memory_space=pltpu.VMEM)
    return pl.pallas_call(
        join_kernel,
        out_shape=jax.ShapeDtypeStruct((512, 128), BF16),
        in_specs=[vmem, vmem],
        out_specs=vmem,
        compiler_params=pltpu.CompilerParams(vmem_limit_bytes=LIMIT),
        name="join",
    )(first, second)


def carry_kernel(*refs):
    count = len(refs) // 2
    for in_ref, out_ref in zip(refs[:count], refs[count:]):
        out_ref[...] = in_ref[...]


def carry(*arrays):
    vmem = pl.BlockSpec(memory_space=pltpu.VMEM)
    return pl.pallas_call(
        carry_kernel,
        out_shape=[jax.ShapeDtypeStruct(a.shape, a.dtype) for a in arrays],
        in_specs=[vmem] * len(arrays),
        out_specs=[vmem] * len(arrays),
        compiler_params=pltpu.CompilerParams(vmem_limit_bytes=LIMIT),
        name="carry",
    )(*arrays)


def fence(x):
    anywhere = pl.BlockSpec(memory_space=pl.ANY)
    return pl.pallas_call(
        lambda in_ref, out_ref: None,
        out_shape=jax.ShapeDtypeStruct(x.shape, x.dtype),
        in_specs=[anywhere],
        out_specs=anywhere,
        input_output_aliases={0: 0},
        compiler_params=pltpu.CompilerParams(vmem_limit_bytes=LIMIT),
        name="fence",
    )(x)


def shift(x, axes, count, by):
    return lax.ppermute(x, axes, [(i, (i + by) % count) for i in range(count)])


def swap(x, axis):
    return lax.ppermute(x, axis, [(0, 1), (1, 0)])


def body(occ, vir, occ_decay, vir_decay):
    row = lax.axis_index(ROW).astype(jnp.int32).reshape(1)
    col = lax.axis_index(COL).astype(jnp.int32).reshape(1)
    place = [lax.axis_index(a).astype(jnp.int32).reshape(1) for a in ("c", "z0", "xl", Y)]
    scattered = prepare(row, col, occ_decay, vir_decay, occ, vir)
    scattered = lax.all_to_all(scattered, ("c", *COL), 0, 0, tiled=True)
    kept, sent = divide(place[0], occ, vir)
    other = swap(sent, "c")
    arrived = lax.all_to_all(pack(place[0], kept, other, scattered), ("xh", *Z), 0, 0, tiled=True)

    def by_group(first, count):
        parts = [arrived[:, start : start + 8 * count] for start in first]
        parts = jnp.stack([part.reshape(16, count, 8, 128) for part in parts])
        return jnp.transpose(parts, (2, 0, 1, 3, 4)).reshape(256 * count, 128)

    near = jnp.concatenate([by_group((96, 112), 1), by_group((104, 120), 1)], axis=0)
    near = [near]
    for by in (1, 2, 3):
        near.append(shift(near[0], Y, 4, by))
    up = join(near[0], near[1])
    up = shift(up, ("xh", "xl"), 4, 1)
    down = join(near[2], near[3])
    down = shift(down, ("xh", "xl"), 4, -1)

    own = jnp.concatenate([by_group((0, 48), 4), by_group((32, 80), 2)], axis=0)
    across = swap(own, "z0")
    beside = swap(own, "c")
    beside = fence(beside)
    opposite = swap(across, "c")
    points = (own, beside, across, opposite)
    messages = polar_messages(*place, *points, *near, up, down, *c_table())

    received = lax.all_to_all(messages, LAST, 0, 0, tiled=True)
    tables = carry(*a_table(), *b_table())
    return finish(received, *tables)


def solution(mesh):
    fine = Mesh(mesh.devices.reshape((2,) * len(FINE)), FINE)
    return jax.shard_map(
        body,
        mesh=fine,
        in_specs=(P(ROW, COL), P(ROW, COL), P(), P()),
        out_specs=(P(ROW, COL, None), P(ROW, COL, None)),
        check_vma=False,
    )
```

```python
import math

import jax
import jax.numpy as jnp
import numpy as np
from jax import lax
from jax.experimental import pallas as pl
from jax.experimental.pallas import tpu as pltpu
from jax.sharding import Mesh, PartitionSpec as P


NOCC = 1024
NVIR = 512
NGRID = 32768
POLAR_FACTOR = -1.0 / math.sqrt(NOCC * NVIR)
NORMAL = 1.0 / math.sqrt(NGRID)
Z = ("z2", "z1", "z0")
Y = ("y1", "y0")
ROW = ("xh", *Z, "c")
COL = ("xl", *Y)
FINE = ROW + COL
LAST = ("z1", "xl", "y0", "z2", "xh", "y1")
BF16 = jnp.bfloat16
F32 = jnp.float32
LIMIT = 16 * 1024 * 1024


def place_in_last(m, j):
    bits = dict(zip(("xh", "z2", "z1"), ((m >> 2) & 1, (m >> 1) & 1, m & 1)))
    bits.update(zip(COL, ((j >> 2) & 1, (j >> 1) & 1, j & 1)))
    place = 0
    for axis in LAST:
        place = 2 * place + bits[axis]
    return place


def split_table(table):
    high = table.astype(np.float32).astype(jnp.bfloat16)
    low = (table - high.astype(np.float64)).astype(np.float32).astype(jnp.bfloat16)
    return high, low


def rotation(phase):
    cosine, sine = np.cos(phase), np.sin(phase)
    return np.array([[cosine, sine], [-sine, cosine]])


def c_table():
    kc = np.arange(32).reshape(8, 4)
    turn = rotation(2 * np.pi * (kc[..., None] * np.arange(32) % 32) / 32)[:, 0]
    full = np.einsum("pjic,bd->ijpbdc", turn, np.eye(8))
    return split_table(full.reshape(512, 256))


def a_table():
    ka = np.arange(32)
    turn = rotation(2 * np.pi * (ka[:, None] * ka[None, :] % 32) / 32)
    turn = turn.reshape(2, 2, 8, 4, 8, 4)
    full = np.einsum("pqghck,bd->ghpbkcqd", turn, np.eye(8))
    return split_table(full.reshape(512, 512))


def b_table():
    kb = np.arange(32)
    turn = rotation(2 * np.pi * (kb[:, None] * kb[None, :] % 32) / 32) * NORMAL
    turn = turn.reshape(2, 2, 32, 4, 8)
    full = np.einsum("pqkBb,hj->Bhqbpjk", turn, np.eye(4))
    return split_table(full.reshape(256, 256))


def dot(a, b):
    return lax.dot_general(a, b, (((1,), (0,)), ((), ())), preferred_element_type=F32)


def prepare_kernel(row_ref, col_ref, *refs):
    @pl.when(col_ref[0] == 0)
    def _():
        prepare_rows(row_ref[0], *refs)


def prepare_rows(
    row, occ_decay_ref, vir_decay_ref, occ_hbm, vir_hbm, *refs
):
    out_hbm, (occ_ref, vir_ref, out_ref, sems) = refs[:4], refs[4:]
    copies = [
        pltpu.make_async_copy(occ_hbm.at[:, :1024], occ_ref, sems.at[0]),
        pltpu.make_async_copy(vir_hbm.at[:, :1024], vir_ref, sems.at[1]),
    ]
    for copy in copies:
        copy.start()
    for copy in copies:
        copy.wait()

    def column(decay_ref, count):
        index = lax.broadcasted_iota(jnp.int32, (count, 128), 0)
        out = jnp.zeros((count, 128), F32)
        for i in range(count):
            out = jnp.where(index == i, decay_ref[row * count + i], out)
        return out

    def scaled_tiles(ref, decay):
        tiles = [ref[:, 128 * t : 128 * (t + 1)].astype(F32) * decay for t in range(8)]
        return [
            [
                jnp.concatenate(
                    [tiles[4 * t + u][:, 32 * kind : 32 * (kind + 1)] for u in range(4)], axis=1
                )
                for kind in range(4)
            ]
            for t in range(2)
        ]

    occ = scaled_tiles(occ_ref, column(occ_decay_ref, 32))
    vir = scaled_tiles(vir_ref, column(vir_decay_ref, 16))
    for y1 in range(2):
        for t in range(2):
            for core in range(2):
                pieces = []
                for z0 in range(2):
                    kind = 2 * z0 + core
                    pieces.append(occ[t][kind][8 * y1 : 8 * (y1 + 1)])
                    pieces.append(occ[t][kind][8 * (2 + y1) : 8 * (3 + y1)])
                    pieces.append(vir[t][kind][8 * y1 : 8 * (y1 + 1)])
                out_ref[2 * y1 + t, core] = jnp.concatenate(pieces, axis=0).astype(BF16)
    results = [
        pltpu.make_async_copy(out_ref.at[y], out_hbm[y], sems.at[2 + y]) for y in range(4)
    ]
    for result in results:
        result.start()
    for result in results:
        result.wait()


def prepare(row, col, occ_decay, vir_decay, occ, vir):
    smem = pl.BlockSpec(memory_space=pltpu.SMEM)
    hbm = pl.BlockSpec(memory_space=pl.ANY)
    return pl.pallas_call(
        prepare_kernel,
        out_shape=[jax.ShapeDtypeStruct((2, 48, 128), BF16)] * 4,
        in_specs=[smem] * 4 + [hbm] * 2,
        out_specs=[hbm] * 4,
        scratch_shapes=[
            pltpu.VMEM((32, 1024), BF16),
            pltpu.VMEM((16, 1024), BF16),
            pltpu.VMEM((4, 2, 48, 128), BF16),
            pltpu.SemaphoreType.DMA((6,)),
        ],
        name="prepare",
    )(row, col, occ_decay, vir_decay, occ, vir)


def divide_kernel(core_ref, occ_ref, vir_ref, kept_ref, sent_ref):
    core = core_ref[0]
    for out_ref, which in ((kept_ref, core), (sent_ref, 1 - core)):
        for p in range(16):
            lanes = pl.ds(pl.multiple_of(128 * (2 * p + which), 128), 128)
            out_ref[p, :32, :] = occ_ref[:, lanes]
            out_ref[p, 32:, :] = vir_ref[:, lanes]


def divide(core, occ, vir):
    vmem = pl.BlockSpec(memory_space=pltpu.VMEM)
    shape = jax.ShapeDtypeStruct((16, 48, 128), BF16)
    return pl.pallas_call(
        divide_kernel,
        out_shape=(shape, shape),
        in_specs=[pl.BlockSpec(memory_space=pltpu.SMEM), vmem, vmem],
        out_specs=(vmem, vmem),
        compiler_params=pltpu.CompilerParams(vmem_limit_bytes=LIMIT),
        name="divide",
    )(core, occ, vir)


def call(kernel, out_shapes, scalars, *arrays):
    vmem = pl.BlockSpec(memory_space=pltpu.VMEM)
    smem = pl.BlockSpec(memory_space=pltpu.SMEM)
    return pl.pallas_call(
        kernel,
        out_shape=[jax.ShapeDtypeStruct(shape, BF16) for shape in out_shapes],
        in_specs=[smem] * len(scalars) + [vmem] * len(arrays),
        out_specs=[vmem] * len(out_shapes),
        compiler_params=pltpu.CompilerParams(vmem_limit_bytes=LIMIT),
    )(*scalars, *arrays)


def pack_kernel(core_ref, kept_ref, other_ref, out_ref):
    core = core_ref[0]
    out_ref[:, pl.ds(pl.multiple_of(48 * core, 16), 48), :] = kept_ref[...]
    out_ref[:, pl.ds(pl.multiple_of(48 * (1 - core), 16), 48), :] = other_ref[...]


def choose_y_kernel(y_ref, *refs):
    for y in range(4):

        @pl.when(y_ref[0] == y)
        def _():
            refs[4][...] = refs[y][...]


def choose_x_kernel(xl_ref, core_ref, *refs):
    for xl in range(2):

        @pl.when(xl_ref[0] == xl)
        def _():
            refs[2][...] = refs[xl][core_ref[0]]
            refs[3][...] = refs[xl][1 - core_ref[0]]


def pack_share_kernel(core_ref, kept_ref, other_ref, out_ref):
    for core in range(2):
        for ref, own in ((kept_ref, core), (other_ref, 1 - core)):

            @pl.when(core_ref[0] == own)
            def _():
                for p in range(16):
                    rows = 24 * (p % 2)
                    out_ref[p, 24 * core : 24 * (core + 1), :] = ref[rows : rows + 24, :]


def polar_kernel(core_ref, z0_ref, y_ref, *refs):
    points, near, (high_ref, low_ref) = refs[:4], refs[4:8], refs[8:10]
    out_ref, polar_ref, occ_ref, vir_ref = refs[-4:]
    core, z0, y = core_ref[0], z0_ref[0], y_ref[0]
    for step in range(4):
        chunk = lax.rem(y + 4 - step, 4)
        y1, y0 = lax.div(chunk, 2), lax.rem(chunk, 2)
        lanes = pl.ds(pl.multiple_of(128 * y0, 128), 128)

        def rows(group):
            return pl.ds(pl.multiple_of(256 * group, 256), 256)

        occ_ref[rows(y1), lanes] = near[step][:256]
        occ_ref[rows(2 + y1), lanes] = near[step][256:512]
        vir_ref[rows(y1), lanes] = near[step][512:]
    occ = jnp.concatenate([ref[:1024].T for ref in points], axis=0)
    vir = jnp.concatenate([ref[1024:].T for ref in points], axis=0)
    product = dot(occ, occ_ref[...]) * dot(vir, vir_ref[...]) * POLAR_FACTOR
    for k in range(4):
        place = 2 * (z0 if k < 2 else 1 - z0) + (core if k % 2 == 0 else 1 - core)
        polar_ref[pl.ds(pl.multiple_of(128 * place, 128), 128), :] = product[
            128 * k : 128 * (k + 1)
        ]
    for half in range(2):
        polar = polar_ref[256 * half : 256 * (half + 1), :]
        polar_high = polar.astype(BF16)
        polar_low = (polar - polar_high.astype(F32)).astype(BF16)
        spectrum = (
            dot(high_ref[...], polar_high)
            + dot(high_ref[...], polar_low)
            + dot(low_ref[...], polar_high)
        )
        for m in range(8):
            pieces = [spectrum[128 * i : 128 * (i + 1), 32 * m : 32 * (m + 1)] for i in range(4)]
            message = jnp.concatenate(pieces, axis=1).astype(BF16)
            for j in range(8):
                out_ref[place_in_last(m, j), half] = message[16 * j : 16 * (j + 1)]


def polar_messages(*arrays):
    vmem = pl.BlockSpec(memory_space=pltpu.VMEM)
    return pl.pallas_call(
        polar_kernel,
        out_shape=jax.ShapeDtypeStruct((64, 2, 16, 128), BF16),
        in_specs=[pl.BlockSpec(memory_space=pltpu.SMEM)] * 3 + [vmem] * 10,
        out_specs=vmem,
        scratch_shapes=[
            pltpu.VMEM((512, 256), F32),
            pltpu.VMEM((1024, 256), BF16),
            pltpu.VMEM((512, 256), BF16),
        ],
        compiler_params=pltpu.CompilerParams(vmem_limit_bytes=LIMIT),
        name="polar",
    )(*arrays)


def finish_kernel(x_ref, a_high_ref, a_low_ref, b_high_ref, b_low_ref, *refs):
    outs, parts, sems = refs[:2], refs[2:4], refs[4]
    x = jnp.concatenate(
        [
            jnp.concatenate(
                [x_ref[place_in_last(2 * k + block // 2, j), block % 2] for k in range(4) for j in range(8)],
                axis=0,
            )
            for block in range(4)
        ],
        axis=1,
    )
    planes = dot(a_high_ref[...], x) + dot(a_low_ref[...], x)
    copies = []
    for part in range(4):
        z = jnp.concatenate(
            [
                jnp.concatenate(
                    [
                        planes[64 * g : 64 * (g + 1), 128 * block : 128 * (block + 1)]
                        for block in range(4)
                    ],
                    axis=0,
                ).T
                for g in (2 * part, 2 * part + 1)
            ],
            axis=0,
        )
        z_high = z.astype(BF16)
        z_low = (z - z_high.astype(F32)).astype(BF16)
        out = (
            dot(z_high, b_high_ref[...])
            + dot(z_high, b_low_ref[...])
            + dot(z_low, b_high_ref[...])
        )
        for which in range(2):
            for g in range(2):
                for i in range(4):
                    rows = 128 * g + 32 * i
                    parts[which][:, i, 128 * (2 * part + g) : 128 * (2 * part + g + 1)] = out[
                        rows : rows + 32, 128 * which : 128 * (which + 1)
                    ]
            lanes = pl.ds(256 * part, 256)
            copy = pltpu.make_async_copy(
                parts[which].at[:, :, lanes], outs[which].at[:, :, lanes], sems.at[which, part]
            )
            copy.start()
            copies.append(copy)
    for copy in copies:
        copy.wait()


def finish(x, *tables):
    vmem = pl.BlockSpec(memory_space=pltpu.VMEM)
    hbm = pl.BlockSpec(memory_space=pl.ANY)
    shape = jax.ShapeDtypeStruct((32, 4, 1024), F32)
    return pl.pallas_call(
        finish_kernel,
        out_shape=(shape, shape),
        in_specs=[vmem] * 5,
        out_specs=(hbm, hbm),
        scratch_shapes=[
            pltpu.VMEM((32, 4, 1024), F32),
            pltpu.VMEM((32, 4, 1024), F32),
            pltpu.SemaphoreType.DMA((2, 4)),
        ],
        compiler_params=pltpu.CompilerParams(vmem_limit_bytes=LIMIT),
        name="finish",
    )(x, *tables)


def carry_kernel(*refs):
    count = len(refs) // 2
    for in_ref, out_ref in zip(refs[:count], refs[count:]):
        out_ref[...] = in_ref[...]


def carry(*arrays):
    vmem = pl.BlockSpec(memory_space=pltpu.VMEM)
    return pl.pallas_call(
        carry_kernel,
        out_shape=[jax.ShapeDtypeStruct(a.shape, a.dtype) for a in arrays],
        in_specs=[vmem] * len(arrays),
        out_specs=[vmem] * len(arrays),
        compiler_params=pltpu.CompilerParams(vmem_limit_bytes=LIMIT),
        name="carry",
    )(*arrays)


def fence(x):
    anywhere = pl.BlockSpec(memory_space=pl.ANY)
    return pl.pallas_call(
        lambda in_ref, out_ref: None,
        out_shape=jax.ShapeDtypeStruct(x.shape, x.dtype),
        in_specs=[anywhere],
        out_specs=anywhere,
        input_output_aliases={0: 0},
        compiler_params=pltpu.CompilerParams(vmem_limit_bytes=LIMIT),
        name="fence",
    )(x)


def shift(x, axes, count, by):
    return lax.ppermute(x, axes, [(i, (i + by) % count) for i in range(count)])


def swap(x, axis):
    return lax.ppermute(x, axis, [(0, 1), (1, 0)])


def by_group(part, first, count):
    parts = [part[:, start : start + 8 * count] for start in first]
    parts = jnp.stack([part.reshape(16, count, 8, 128) for part in parts])
    return jnp.transpose(parts, (2, 0, 1, 3, 4)).reshape(256 * count, 128)


def body(occ, vir, occ_decay, vir_decay):
    def index(axes):
        return lax.axis_index(axes).astype(jnp.int32).reshape(1)

    core, xl, y = index("c"), index("xl"), index(Y)

    kept, sent = divide(core, occ, vir)
    other = swap(sent, "c")
    packed = call(pack_kernel, [(16, 96, 128)], [core], kept, other)[0]
    arrived = lax.all_to_all(packed, ("xh", *Z), 0, 0, tiled=True)

    pieces = list(prepare(index(ROW), index(COL), occ_decay, vir_decay, occ, vir))
    for by in (1, 2, 3):
        pieces[by] = lax.ppermute(pieces[by], COL, [(0, by)])
    piece = call(choose_y_kernel, [(2, 48, 128)], [y], *pieces)[0]
    handed = lax.ppermute(piece, COL, [(k, 4 + k) for k in range(4)])
    shapes = [(48, 128)] * 2
    kept, sent = call(choose_x_kernel, shapes, [xl, core], piece, handed)
    other = swap(sent, "c")
    share = call(pack_share_kernel, [(16, 48, 128)], [core], kept, other)[0]
    share = lax.all_to_all(share, ("xh", *Z), 0, 0, tiled=True)

    parts = [by_group(share, (8 * k, 24 + 8 * k), 1) for k in range(3)]
    near = [jnp.concatenate(parts, axis=0)]
    for by in (1, 2, 3):
        near.append(shift(near[0], Y, 4, by))

    own = jnp.concatenate([by_group(arrived, (0, 48), 4), by_group(arrived, (32, 80), 2)], axis=0)
    across = swap(own, "z0")
    beside = swap(own, "c")
    beside = fence(beside)
    opposite = swap(across, "c")
    points = (own, beside, across, opposite)
    place = (core, index("z0"), y)
    messages = polar_messages(*place, *points, *near, *c_table())
    received = lax.all_to_all(messages, LAST, 0, 0, tiled=True)
    tables = carry(*a_table(), *b_table())
    return finish(received, *tables)


def solution(mesh):
    fine = Mesh(mesh.devices.reshape((2,) * len(FINE)), FINE)
    return jax.shard_map(
        body,
        mesh=fine,
        in_specs=(P(ROW, COL), P(ROW, COL), P(), P()),
        out_specs=(P(ROW, COL, None), P(ROW, COL, None)),
        check_vma=False,
    )
```

```python
import math

import jax
import jax.numpy as jnp
import numpy as np
from jax import lax
from jax.experimental import pallas as pl
from jax.experimental.pallas import tpu as pltpu
from jax.sharding import Mesh, PartitionSpec as P


NOCC = 1024
NVIR = 512
NGRID = 32768
POLAR_FACTOR = -1.0 / math.sqrt(NOCC * NVIR)
NORMAL = 1.0 / math.sqrt(NGRID)
Z = ("z2", "z1", "z0")
Y = ("y1", "y0")
ROW = ("xh", *Z, "c")
COL = ("xl", *Y)
FINE = ROW + COL
LAST = ("z1", "xl", "y0", "z2", "xh", "y1")
BF16 = jnp.bfloat16
F32 = jnp.float32
LIMIT = 16 * 1024 * 1024


def place_in_last(m, j):
    bits = dict(zip(("xh", "z2", "z1"), ((m >> 2) & 1, (m >> 1) & 1, m & 1)))
    bits.update(zip(COL, ((j >> 2) & 1, (j >> 1) & 1, j & 1)))
    place = 0
    for axis in LAST:
        place = 2 * place + bits[axis]
    return place


def split_table(table):
    high = table.astype(np.float32).astype(jnp.bfloat16)
    low = (table - high.astype(np.float64)).astype(np.float32).astype(jnp.bfloat16)
    return high, low


def rotation(phase):
    cosine, sine = np.cos(phase), np.sin(phase)
    return np.array([[cosine, sine], [-sine, cosine]])


def c_table():
    kc = np.arange(32).reshape(8, 4)
    turn = rotation(2 * np.pi * (kc[..., None] * np.arange(32) % 32) / 32)[:, 0]
    full = np.einsum("pjic,bd->ijpbdc", turn, np.eye(8))
    return split_table(full.reshape(512, 256))


def a_table():
    ka = np.arange(32)
    turn = rotation(2 * np.pi * (ka[:, None] * ka[None, :] % 32) / 32)
    turn = turn.reshape(2, 2, 8, 4, 8, 4)
    full = np.einsum("pqghck,bd->ghpbkcqd", turn, np.eye(8))
    return split_table(full.reshape(512, 512))


def b_table():
    kb = np.arange(32)
    turn = rotation(2 * np.pi * (kb[:, None] * kb[None, :] % 32) / 32) * NORMAL
    turn = turn.reshape(2, 2, 32, 4, 8)
    full = np.einsum("pqkBb,hj->Bhqbpjk", turn, np.eye(4))
    return split_table(full.reshape(256, 256))


def dot(a, b):
    return lax.dot_general(a, b, (((1,), (0,)), ((), ())), preferred_element_type=F32)


def prepare_kernel(row_ref, col_ref, *refs):
    @pl.when(col_ref[0] == 0)
    def _():
        prepare_rows(row_ref[0], *refs)


def prepare_rows(
    row, occ_decay_ref, vir_decay_ref, occ_hbm, vir_hbm, out_hbm, occ_ref, vir_ref, out_ref, sems
):
    copies = [
        pltpu.make_async_copy(occ_hbm.at[:, :1024], occ_ref, sems.at[0]),
        pltpu.make_async_copy(vir_hbm.at[:, :1024], vir_ref, sems.at[1]),
    ]
    for copy in copies:
        copy.start()
    for copy in copies:
        copy.wait()

    def column(decay_ref, count):
        index = lax.broadcasted_iota(jnp.int32, (count, 128), 0)
        out = jnp.zeros((count, 128), F32)
        for i in range(count):
            out = jnp.where(index == i, decay_ref[row * count + i], out)
        return out

    def scaled_tiles(ref, decay):
        tiles = [ref[:, 128 * t : 128 * (t + 1)].astype(F32) * decay for t in range(8)]
        return [
            [
                jnp.concatenate(
                    [tiles[4 * t + u][:, 32 * kind : 32 * (kind + 1)] for u in range(4)], axis=1
                )
                for kind in range(4)
            ]
            for t in range(2)
        ]

    occ = scaled_tiles(occ_ref, column(occ_decay_ref, 32))
    vir = scaled_tiles(vir_ref, column(vir_decay_ref, 16))
    for y1 in range(2):
        for t in range(2):
            for kind in range(4):
                piece = jnp.concatenate(
                    [
                        occ[t][kind][8 * y1 : 8 * (y1 + 1)],
                        occ[t][kind][8 * (2 + y1) : 8 * (3 + y1)],
                        vir[t][kind][8 * y1 : 8 * (y1 + 1)],
                    ],
                    axis=0,
                ).astype(BF16)
                for xl in range(2):
                    out_ref[8 * (kind % 2) + 4 * xl + 2 * y1 + t, kind // 2] = piece
    result = pltpu.make_async_copy(out_ref, out_hbm, sems.at[2])
    result.start()
    result.wait()


def prepare(row, col, occ_decay, vir_decay, occ, vir):
    smem = pl.BlockSpec(memory_space=pltpu.SMEM)
    hbm = pl.BlockSpec(memory_space=pl.ANY)
    return pl.pallas_call(
        prepare_kernel,
        out_shape=jax.ShapeDtypeStruct((16, 2, 24, 128), BF16),
        in_specs=[smem] * 4 + [hbm] * 2,
        out_specs=hbm,
        scratch_shapes=[
            pltpu.VMEM((32, 1024), BF16),
            pltpu.VMEM((16, 1024), BF16),
            pltpu.VMEM((16, 2, 24, 128), BF16),
            pltpu.SemaphoreType.DMA((3,)),
        ],
        name="prepare",
    )(row, col, occ_decay, vir_decay, occ, vir)


def divide_kernel(core_ref, occ_ref, vir_ref, kept_ref, sent_ref):
    core = core_ref[0]
    for out_ref, which in ((kept_ref, core), (sent_ref, 1 - core)):
        for p in range(16):
            lanes = pl.ds(pl.multiple_of(128 * (2 * p + which), 128), 128)
            out_ref[p, :32, :] = occ_ref[:, lanes]
            out_ref[p, 32:, :] = vir_ref[:, lanes]


def divide(core, occ, vir):
    vmem = pl.BlockSpec(memory_space=pltpu.VMEM)
    shape = jax.ShapeDtypeStruct((16, 48, 128), BF16)
    return pl.pallas_call(
        divide_kernel,
        out_shape=(shape, shape),
        in_specs=[pl.BlockSpec(memory_space=pltpu.SMEM), vmem, vmem],
        out_specs=(vmem, vmem),
        compiler_params=pltpu.CompilerParams(vmem_limit_bytes=LIMIT),
        name="divide",
    )(core, occ, vir)


def pack_kernel(core_ref, kept_ref, other_ref, rows_ref, out_ref):
    core = core_ref[0]
    out_ref[:, pl.ds(pl.multiple_of(48 * core, 16), 48), :] = kept_ref[...]
    out_ref[:, pl.ds(pl.multiple_of(48 * (1 - core), 16), 48), :] = other_ref[...]
    for p in range(16):
        out_ref[p, 96:120, :] = rows_ref[0, p % 2]
        out_ref[p, 120:144, :] = rows_ref[8, p % 2]


def pack(core, kept, other, rows):
    vmem = pl.BlockSpec(memory_space=pltpu.VMEM)
    return pl.pallas_call(
        pack_kernel,
        out_shape=jax.ShapeDtypeStruct((16, 144, 128), BF16),
        in_specs=[pl.BlockSpec(memory_space=pltpu.SMEM)] + [vmem] * 3,
        out_specs=vmem,
        compiler_params=pltpu.CompilerParams(vmem_limit_bytes=LIMIT),
        name="pack",
    )(core, kept, other, rows)


def polar_kernel(core_ref, z0_ref, y_ref, *refs):
    points, near, (high_ref, low_ref) = refs[:4], refs[4:8], refs[8:10]
    out_hbm, polar_ref, occ_ref, vir_ref, out_ref, sems = refs[10:]
    copies = []
    core, z0, y = core_ref[0], z0_ref[0], y_ref[0]
    for step in range(4):
        chunk = lax.rem(y + 4 - step, 4)
        y1, y0 = lax.div(chunk, 2), lax.rem(chunk, 2)
        lanes = pl.ds(pl.multiple_of(128 * y0, 128), 128)

        def rows(group):
            return pl.ds(pl.multiple_of(256 * group, 256), 256)

        occ_ref[rows(y1), lanes] = near[step][:256]
        occ_ref[rows(2 + y1), lanes] = near[step][256:512]
        vir_ref[rows(y1), lanes] = near[step][512:]
    occ = jnp.concatenate([ref[:1024].T for ref in points], axis=0)
    vir = jnp.concatenate([ref[1024:].T for ref in points], axis=0)
    product = dot(occ, occ_ref[...]) * dot(vir, vir_ref[...]) * POLAR_FACTOR
    for k in range(4):
        place = 2 * (z0 if k < 2 else 1 - z0) + (core if k % 2 == 0 else 1 - core)
        polar_ref[pl.ds(pl.multiple_of(128 * place, 128), 128), :] = product[
            128 * k : 128 * (k + 1)
        ]
    for half in range(2):
        polar = polar_ref[256 * half : 256 * (half + 1), :]
        polar_high = polar.astype(BF16)
        polar_low = (polar - polar_high.astype(F32)).astype(BF16)
        spectrum = (
            dot(high_ref[...], polar_high)
            + dot(high_ref[...], polar_low)
            + dot(low_ref[...], polar_high)
        )
        for m in range(8):
            pieces = [spectrum[128 * i : 128 * (i + 1), 32 * m : 32 * (m + 1)] for i in range(4)]
            message = jnp.concatenate(pieces, axis=1).astype(BF16)
            for j in range(8):
                out_ref[half, place_in_last(m, j)] = message[16 * j : 16 * (j + 1)]
        copy = pltpu.make_async_copy(out_ref.at[half], out_hbm.at[:, half], sems.at[half])
        copy.start()
        copies.append(copy)
    for copy in copies:
        copy.wait()


def polar_messages(*arrays):
    vmem = pl.BlockSpec(memory_space=pltpu.VMEM)
    return pl.pallas_call(
        polar_kernel,
        out_shape=jax.ShapeDtypeStruct((64, 2, 16, 128), BF16),
        in_specs=[pl.BlockSpec(memory_space=pltpu.SMEM)] * 3 + [vmem] * 10,
        out_specs=pl.BlockSpec(memory_space=pl.ANY),
        scratch_shapes=[
            pltpu.VMEM((512, 256), F32),
            pltpu.VMEM((1024, 256), BF16),
            pltpu.VMEM((512, 256), BF16),
            pltpu.VMEM((2, 64, 16, 128), BF16),
            pltpu.SemaphoreType.DMA((2,)),
        ],
        compiler_params=pltpu.CompilerParams(vmem_limit_bytes=LIMIT),
        name="polar",
    )(*arrays)


def finish_kernel(x_ref, a_high_ref, a_low_ref, b_high_ref, b_low_ref, *refs):
    outs, parts, sems = refs[:2], refs[2:4], refs[4]
    x = jnp.concatenate(
        [
            jnp.concatenate(
                [x_ref[place_in_last(2 * k + block // 2, j), block % 2] for k in range(4) for j in range(8)],
                axis=0,
            )
            for block in range(4)
        ],
        axis=1,
    )
    planes = dot(a_high_ref[...], x) + dot(a_low_ref[...], x)
    copies = []
    for part in range(4):
        z = jnp.concatenate(
            [
                jnp.concatenate(
                    [
                        planes[64 * g : 64 * (g + 1), 128 * block : 128 * (block + 1)]
                        for block in range(4)
                    ],
                    axis=0,
                ).T
                for g in (2 * part, 2 * part + 1)
            ],
            axis=0,
        )
        z_high = z.astype(BF16)
        z_low = (z - z_high.astype(F32)).astype(BF16)
        out = (
            dot(z_high, b_high_ref[...])
            + dot(z_high, b_low_ref[...])
            + dot(z_low, b_high_ref[...])
        )
        for which in range(2):
            for g in range(2):
                for i in range(4):
                    rows = 128 * g + 32 * i
                    parts[which][:, i, 128 * (2 * part + g) : 128 * (2 * part + g + 1)] = out[
                        rows : rows + 32, 128 * which : 128 * (which + 1)
                    ]
            lanes = pl.ds(256 * part, 256)
            copy = pltpu.make_async_copy(
                parts[which].at[:, :, lanes], outs[which].at[:, :, lanes], sems.at[which, part]
            )
            copy.start()
            copies.append(copy)
    for copy in copies:
        copy.wait()


def finish(x, *tables):
    vmem = pl.BlockSpec(memory_space=pltpu.VMEM)
    hbm = pl.BlockSpec(memory_space=pl.ANY)
    shape = jax.ShapeDtypeStruct((32, 4, 1024), F32)
    return pl.pallas_call(
        finish_kernel,
        out_shape=(shape, shape),
        in_specs=[vmem] * 5,
        out_specs=(hbm, hbm),
        scratch_shapes=[
            pltpu.VMEM((32, 4, 1024), F32),
            pltpu.VMEM((32, 4, 1024), F32),
            pltpu.SemaphoreType.DMA((2, 4)),
        ],
        compiler_params=pltpu.CompilerParams(vmem_limit_bytes=LIMIT),
        name="finish",
    )(x, *tables)


def carry_kernel(*refs):
    count = len(refs) // 2
    for in_ref, out_ref in zip(refs[:count], refs[count:]):
        out_ref[...] = in_ref[...]


def carry(*arrays):
    vmem = pl.BlockSpec(memory_space=pltpu.VMEM)
    return pl.pallas_call(
        carry_kernel,
        out_shape=[jax.ShapeDtypeStruct(a.shape, a.dtype) for a in arrays],
        in_specs=[vmem] * len(arrays),
        out_specs=[vmem] * len(arrays),
        compiler_params=pltpu.CompilerParams(vmem_limit_bytes=LIMIT),
        name="carry",
    )(*arrays)


def fence(x):
    anywhere = pl.BlockSpec(memory_space=pl.ANY)
    return pl.pallas_call(
        lambda in_ref, out_ref: None,
        out_shape=jax.ShapeDtypeStruct(x.shape, x.dtype),
        in_specs=[anywhere],
        out_specs=anywhere,
        input_output_aliases={0: 0},
        compiler_params=pltpu.CompilerParams(vmem_limit_bytes=LIMIT),
        name="fence",
    )(x)


def shift(x, axes, count, by):
    return lax.ppermute(x, axes, [(i, (i + by) % count) for i in range(count)])


def swap(x, axis):
    return lax.ppermute(x, axis, [(0, 1), (1, 0)])


def body(occ, vir, occ_decay, vir_decay):
    row = lax.axis_index(ROW).astype(jnp.int32).reshape(1)
    col = lax.axis_index(COL).astype(jnp.int32).reshape(1)
    place = [lax.axis_index(a).astype(jnp.int32).reshape(1) for a in ("c", "z0", Y)]
    scattered = prepare(row, col, occ_decay, vir_decay, occ, vir)
    scattered = lax.all_to_all(scattered, ("c", *COL), 0, 0, tiled=True)
    kept, sent = divide(place[0], occ, vir)
    other = swap(sent, "c")
    arrived = lax.all_to_all(pack(place[0], kept, other, scattered), ("xh", *Z), 0, 0, tiled=True)

    def by_group(first, count):
        parts = [arrived[:, start : start + 8 * count] for start in first]
        parts = jnp.stack([part.reshape(16, count, 8, 128) for part in parts])
        return jnp.transpose(parts, (2, 0, 1, 3, 4)).reshape(256 * count, 128)

    parts = [by_group((96 + 8 * k, 120 + 8 * k), 1) for k in range(3)]
    near = jnp.concatenate(parts, axis=0)
    near = [near]
    for by in (1, 2, 3):
        near.append(shift(near[0], Y, 4, by))
    own = jnp.concatenate([by_group((0, 48), 4), by_group((32, 80), 2)], axis=0)
    across = swap(own, "z0")
    beside = swap(own, "c")
    beside = fence(beside)
    opposite = swap(across, "c")
    points = (own, beside, across, opposite)
    messages = polar_messages(*place, *points, *near, *c_table())

    received = lax.all_to_all(messages, LAST, 0, 0, tiled=True)
    tables = carry(*a_table(), *b_table())
    return finish(received, *tables)


def solution(mesh):
    fine = Mesh(mesh.devices.reshape((2,) * len(FINE)), FINE)
    return jax.shard_map(
        body,
        mesh=fine,
        in_specs=(P(ROW, COL), P(ROW, COL), P(), P()),
        out_specs=(P(ROW, COL, None), P(ROW, COL, None)),
        check_vma=False,
    )
```

```python
import math

import jax
import jax.numpy as jnp
import numpy as np
from jax import lax
from jax.experimental import pallas as pl
from jax.experimental.pallas import tpu as pltpu
from jax.sharding import Mesh, PartitionSpec as P


NOCC = 1024
NVIR = 512
NGRID = 32768
POLAR_FACTOR = -1.0 / math.sqrt(NOCC * NVIR)
NORMAL = 1.0 / math.sqrt(NGRID)
Z = ("z2", "z1", "z0")
Y = ("y1", "y0")
ROW = ("xh", *Z, "c")
COL = ("xl", *Y)
FINE = ROW + COL
LAST = ("z1", "xl", "y0", "z2", "xh", "y1")
BF16 = jnp.bfloat16
F32 = jnp.float32
LIMIT = 16 * 1024 * 1024


def place_in_last(m, j):
    bits = dict(zip(("xh", "z2", "z1"), ((m >> 2) & 1, (m >> 1) & 1, m & 1)))
    bits.update(zip(COL, ((j >> 2) & 1, (j >> 1) & 1, j & 1)))
    place = 0
    for axis in LAST:
        place = 2 * place + bits[axis]
    return place


def split_table(table):
    high = table.astype(np.float32).astype(jnp.bfloat16)
    low = (table - high.astype(np.float64)).astype(np.float32).astype(jnp.bfloat16)
    return high, low


def rotation(phase):
    cosine, sine = np.cos(phase), np.sin(phase)
    return np.array([[cosine, sine], [-sine, cosine]])


def c_table():
    kc = np.arange(32).reshape(8, 4)
    turn = rotation(2 * np.pi * (kc[..., None] * np.arange(32) % 32) / 32)[:, 0]
    full = np.einsum("pjic,bd->ijpbdc", turn, np.eye(8))
    return split_table(full.reshape(512, 256))


def a_table():
    ka = np.arange(32)
    turn = rotation(2 * np.pi * (ka[:, None] * ka[None, :] % 32) / 32)
    turn = turn.reshape(2, 2, 8, 4, 8, 4)
    full = np.einsum("pqghck,bd->ghpbkcqd", turn, np.eye(8))
    return split_table(full.reshape(512, 512))


def b_table():
    kb = np.arange(32)
    turn = rotation(2 * np.pi * (kb[:, None] * kb[None, :] % 32) / 32) * NORMAL
    turn = turn.reshape(2, 2, 32, 4, 8)
    full = np.einsum("pqkBb,hj->Bhqbpjk", turn, np.eye(4))
    return split_table(full.reshape(256, 256))


def dot(a, b):
    return lax.dot_general(a, b, (((1,), (0,)), ((), ())), preferred_element_type=F32)


def prepare_kernel(row_ref, col_ref, *refs):
    @pl.when(col_ref[0] == 0)
    def _():
        prepare_rows(row_ref[0], *refs)


def prepare_rows(
    row, occ_decay_ref, vir_decay_ref, occ_hbm, vir_hbm, out_hbm, occ_ref, vir_ref, out_ref, sems
):
    copies = [
        pltpu.make_async_copy(occ_hbm.at[:, :1024], occ_ref, sems.at[0]),
        pltpu.make_async_copy(vir_hbm.at[:, :1024], vir_ref, sems.at[1]),
    ]
    for copy in copies:
        copy.start()
    for copy in copies:
        copy.wait()

    def column(decay_ref, count):
        index = lax.broadcasted_iota(jnp.int32, (count, 128), 0)
        out = jnp.zeros((count, 128), F32)
        for i in range(count):
            out = jnp.where(index == i, decay_ref[row * count + i], out)
        return out

    def scaled_tiles(ref, decay):
        tiles = [ref[:, 128 * t : 128 * (t + 1)].astype(F32) * decay for t in range(8)]
        return [
            [
                jnp.concatenate(
                    [tiles[4 * t + u][:, 32 * kind : 32 * (kind + 1)] for u in range(4)], axis=1
                )
                for kind in range(4)
            ]
            for t in range(2)
        ]

    occ = scaled_tiles(occ_ref, column(occ_decay_ref, 32))
    vir = scaled_tiles(vir_ref, column(vir_decay_ref, 16))
    for y1 in range(2):
        for t in range(2):
            for kind in range(4):
                piece = jnp.concatenate(
                    [
                        occ[t][kind][8 * y1 : 8 * (y1 + 1)],
                        occ[t][kind][8 * (2 + y1) : 8 * (3 + y1)],
                        vir[t][kind][8 * y1 : 8 * (y1 + 1)],
                    ],
                    axis=0,
                ).astype(BF16)
                for xl in range(2):
                    out_ref[4 * xl + 2 * y1 + t, kind] = piece
    result = pltpu.make_async_copy(out_ref, out_hbm, sems.at[2])
    result.start()
    result.wait()


def prepare(row, col, occ_decay, vir_decay, occ, vir):
    smem = pl.BlockSpec(memory_space=pltpu.SMEM)
    hbm = pl.BlockSpec(memory_space=pl.ANY)
    return pl.pallas_call(
        prepare_kernel,
        out_shape=jax.ShapeDtypeStruct((8, 4, 24, 128), BF16),
        in_specs=[smem] * 4 + [hbm] * 2,
        out_specs=hbm,
        scratch_shapes=[
            pltpu.VMEM((32, 1024), BF16),
            pltpu.VMEM((16, 1024), BF16),
            pltpu.VMEM((8, 4, 24, 128), BF16),
            pltpu.SemaphoreType.DMA((3,)),
        ],
        name="prepare",
    )(row, col, occ_decay, vir_decay, occ, vir)


def pack_kernel(occ_ref, vir_ref, rows_ref, out_ref):
    for p in range(32):
        out_ref[p, 0:32, :] = occ_ref[:, 128 * p : 128 * (p + 1)]
        out_ref[p, 32:48, :] = vir_ref[:, 128 * p : 128 * (p + 1)]
        out_ref[p, 48:72, :] = rows_ref[0, p % 4]


def pack(occ, vir, rows):
    vmem = pl.BlockSpec(memory_space=pltpu.VMEM)
    return pl.pallas_call(
        pack_kernel,
        out_shape=jax.ShapeDtypeStruct((32, 72, 128), BF16),
        in_specs=[vmem] * 3,
        out_specs=vmem,
        compiler_params=pltpu.CompilerParams(vmem_limit_bytes=LIMIT),
        name="pack",
    )(occ, vir, rows)


def polar_kernel(core_ref, z0_ref, y_ref, *refs):
    points, near, (high_ref, low_ref) = refs[:4], refs[4:8], refs[8:10]
    out_ref, polar_ref, occ_ref, vir_ref = refs[-4:]
    core, z0, y = core_ref[0], z0_ref[0], y_ref[0]
    for step in range(4):
        chunk = lax.rem(y + 4 - step, 4)
        y1, y0 = lax.div(chunk, 2), lax.rem(chunk, 2)
        lanes = pl.ds(pl.multiple_of(128 * y0, 128), 128)

        def rows(group):
            return pl.ds(pl.multiple_of(256 * group, 256), 256)

        occ_ref[rows(y1), lanes] = near[step][:256]
        occ_ref[rows(2 + y1), lanes] = near[step][256:512]
        vir_ref[rows(y1), lanes] = near[step][512:]
    occ = jnp.concatenate([ref[:, :1024] for ref in points], axis=0)
    vir = jnp.concatenate([ref[:, 1024:] for ref in points], axis=0)
    product = dot(occ, occ_ref[...]) * dot(vir, vir_ref[...]) * POLAR_FACTOR
    for k in range(4):
        place = 2 * (z0 if k < 2 else 1 - z0) + (core if k % 2 == 0 else 1 - core)
        polar_ref[pl.ds(pl.multiple_of(128 * place, 128), 128), :] = product[
            128 * k : 128 * (k + 1)
        ]
    for half in range(2):
        polar = polar_ref[256 * half : 256 * (half + 1), :]
        polar_high = polar.astype(BF16)
        polar_low = (polar - polar_high.astype(F32)).astype(BF16)
        spectrum = (
            dot(high_ref[...], polar_high)
            + dot(high_ref[...], polar_low)
            + dot(low_ref[...], polar_high)
        ).astype(BF16)
        for m in range(8):
            pieces = [spectrum[128 * i : 128 * (i + 1), 32 * m : 32 * (m + 1)] for i in range(4)]
            message = jnp.concatenate(pieces, axis=1)
            for j in range(8):
                out_ref[place_in_last(m, j), half] = message[16 * j : 16 * (j + 1)]


def polar_messages(*arrays):
    vmem = pl.BlockSpec(memory_space=pltpu.VMEM)
    return pl.pallas_call(
        polar_kernel,
        out_shape=jax.ShapeDtypeStruct((64, 2, 16, 128), BF16),
        in_specs=[pl.BlockSpec(memory_space=pltpu.SMEM)] * 3 + [vmem] * 10,
        out_specs=vmem,
        scratch_shapes=[
            pltpu.VMEM((512, 256), F32),
            pltpu.VMEM((1024, 256), BF16),
            pltpu.VMEM((512, 256), BF16),
        ],
        compiler_params=pltpu.CompilerParams(vmem_limit_bytes=LIMIT),
        name="polar",
    )(*arrays)


def finish_kernel(x_ref, a_high_ref, a_low_ref, b_high_ref, b_low_ref, *refs):
    outs, parts, sems = refs[:2], refs[2:4], refs[4]
    x = jnp.concatenate(
        [
            jnp.concatenate(
                [x_ref[place_in_last(2 * k + block // 2, j), block % 2] for k in range(4) for j in range(8)],
                axis=0,
            )
            for block in range(4)
        ],
        axis=1,
    )
    planes = dot(a_high_ref[...], x) + dot(a_low_ref[...], x)
    copies = []
    for part in range(4):
        z = jnp.concatenate(
            [
                jnp.concatenate(
                    [
                        planes[64 * g : 64 * (g + 1), 128 * block : 128 * (block + 1)]
                        for block in range(4)
                    ],
                    axis=0,
                ).T
                for g in (2 * part, 2 * part + 1)
            ],
            axis=0,
        )
        z_high = z.astype(BF16)
        z_low = (z - z_high.astype(F32)).astype(BF16)
        out = (
            dot(z_high, b_high_ref[...])
            + dot(z_high, b_low_ref[...])
            + dot(z_low, b_high_ref[...])
        )
        for which in range(2):
            for g in range(2):
                for i in range(4):
                    rows = 128 * g + 32 * i
                    parts[which][:, i, 128 * (2 * part + g) : 128 * (2 * part + g + 1)] = out[
                        rows : rows + 32, 128 * which : 128 * (which + 1)
                    ]
            lanes = pl.ds(256 * part, 256)
            copy = pltpu.make_async_copy(
                parts[which].at[:, :, lanes], outs[which].at[:, :, lanes], sems.at[which, part]
            )
            copy.start()
            copies.append(copy)
    for copy in copies:
        copy.wait()


def finish(x, *tables):
    vmem = pl.BlockSpec(memory_space=pltpu.VMEM)
    hbm = pl.BlockSpec(memory_space=pl.ANY)
    shape = jax.ShapeDtypeStruct((32, 4, 1024), F32)
    return pl.pallas_call(
        finish_kernel,
        out_shape=(shape, shape),
        in_specs=[vmem] * 5,
        out_specs=(hbm, hbm),
        scratch_shapes=[
            pltpu.VMEM((32, 4, 1024), F32),
            pltpu.VMEM((32, 4, 1024), F32),
            pltpu.SemaphoreType.DMA((2, 4)),
        ],
        compiler_params=pltpu.CompilerParams(vmem_limit_bytes=LIMIT),
        name="finish",
    )(x, *tables)


def carry_kernel(*refs):
    count = len(refs) // 2
    for in_ref, out_ref in zip(refs[:count], refs[count:]):
        out_ref[...] = in_ref[...]


def carry(*arrays):
    vmem = pl.BlockSpec(memory_space=pltpu.VMEM)
    return pl.pallas_call(
        carry_kernel,
        out_shape=[jax.ShapeDtypeStruct(a.shape, a.dtype) for a in arrays],
        in_specs=[vmem] * len(arrays),
        out_specs=[vmem] * len(arrays),
        compiler_params=pltpu.CompilerParams(vmem_limit_bytes=LIMIT),
        name="carry",
    )(*arrays)


def turn_kernel(in_ref, out_ref):
    out_ref[...] = in_ref[...].T


def turn(x):
    vmem = pl.BlockSpec(memory_space=pltpu.VMEM)
    return pl.pallas_call(
        turn_kernel,
        out_shape=jax.ShapeDtypeStruct(x.shape[::-1], x.dtype),
        in_specs=[vmem],
        out_specs=vmem,
        compiler_params=pltpu.CompilerParams(vmem_limit_bytes=LIMIT),
        name="turn",
    )(x)


def fence(x):
    anywhere = pl.BlockSpec(memory_space=pl.ANY)
    return pl.pallas_call(
        lambda in_ref, out_ref: None,
        out_shape=jax.ShapeDtypeStruct(x.shape, x.dtype),
        in_specs=[anywhere],
        out_specs=anywhere,
        input_output_aliases={0: 0},
        compiler_params=pltpu.CompilerParams(vmem_limit_bytes=LIMIT),
        name="fence",
    )(x)


def shift(x, axes, count, by):
    return lax.ppermute(x, axes, [(i, (i + by) % count) for i in range(count)])


def swap(x, axis):
    return lax.ppermute(x, axis, [(0, 1), (1, 0)])


def body(occ, vir, occ_decay, vir_decay):
    row = lax.axis_index(ROW).astype(jnp.int32).reshape(1)
    col = lax.axis_index(COL).astype(jnp.int32).reshape(1)
    place = [lax.axis_index(a).astype(jnp.int32).reshape(1) for a in ("c", "z0", Y)]
    scattered = lax.all_to_all(prepare(row, col, occ_decay, vir_decay, occ, vir), COL, 0, 0, tiled=True)
    arrived = lax.all_to_all(pack(occ, vir, scattered), ROW, 0, 0, tiled=True)

    def by_group(part, count):
        part = part.reshape(32, count, 8, 128)
        return jnp.transpose(part, (1, 0, 2, 3)).reshape(256 * count, 128)

    near = jnp.concatenate([by_group(arrived[:, 48:64], 2), by_group(arrived[:, 64:], 1)], axis=0)
    near = [near]
    for by in (1, 2, 3):
        near.append(shift(near[0], Y, 4, by))
    own = jnp.concatenate([by_group(arrived[:, :32], 4), by_group(arrived[:, 32:48], 2)], axis=0)
    own = turn(own)
    across = swap(own, "z0")
    beside = swap(own, "c")
    beside = fence(beside)
    opposite = swap(across, "c")
    points = (own, beside, across, opposite)
    messages = polar_messages(*place, *points, *near, *c_table())

    received = lax.all_to_all(messages, LAST, 0, 0, tiled=True)
    tables = carry(*a_table(), *b_table())
    return finish(received, *tables)


def solution(mesh):
    fine = Mesh(mesh.devices.reshape((2,) * len(FINE)), FINE)
    return jax.shard_map(
        body,
        mesh=fine,
        in_specs=(P(ROW, COL), P(ROW, COL), P(), P()),
        out_specs=(P(ROW, COL, None), P(ROW, COL, None)),
        check_vma=False,
    )
```

```python
import math

import jax
import jax.numpy as jnp
import numpy as np
from jax import lax
from jax.experimental import pallas as pl
from jax.experimental.pallas import tpu as pltpu
from jax.sharding import Mesh, PartitionSpec as P


NOCC = 1024
NVIR = 512
NGRID = 32768
POLAR_FACTOR = -1.0 / math.sqrt(NOCC * NVIR)
NORMAL = 1.0 / math.sqrt(NGRID)
Z = ("z2", "z1", "z0")
Y = ("y1", "y0")
ROW = ("xh", *Z, "c")
COL = ("xl", *Y)
FINE = ROW + COL
LAST = ("z1", "xl", "y0", "z2", "xh", "y1")
BF16 = jnp.bfloat16
F32 = jnp.float32
LIMIT = 16 * 1024 * 1024


def place_in_last(m, j):
    bits = dict(zip(("xh", "z2", "z1"), ((m >> 2) & 1, (m >> 1) & 1, m & 1)))
    bits.update(zip(COL, ((j >> 2) & 1, (j >> 1) & 1, j & 1)))
    place = 0
    for axis in LAST:
        place = 2 * place + bits[axis]
    return place


def split_table(table):
    high = table.astype(np.float32).astype(jnp.bfloat16)
    low = (table - high.astype(np.float64)).astype(np.float32).astype(jnp.bfloat16)
    return high, low


def rotation(phase):
    cosine, sine = np.cos(phase), np.sin(phase)
    return np.array([[cosine, sine], [-sine, cosine]])


def c_table():
    kc = np.arange(32).reshape(8, 4)
    turn = rotation(2 * np.pi * (kc[..., None] * np.arange(32) % 32) / 32)[:, 0]
    full = np.einsum("pjic,bd->ijpbdc", turn, np.eye(8))
    return split_table(full.reshape(512, 256))


def a_table():
    ka = np.arange(32)
    turn = rotation(2 * np.pi * (ka[:, None] * ka[None, :] % 32) / 32)
    turn = turn.reshape(2, 2, 8, 4, 8, 4)
    full = np.einsum("pqghck,bd->ghpbkcqd", turn, np.eye(8))
    return split_table(full.reshape(512, 512))


def b_table():
    kb = np.arange(32)
    turn = rotation(2 * np.pi * (kb[:, None] * kb[None, :] % 32) / 32) * NORMAL
    turn = turn.reshape(2, 2, 32, 4, 8)
    full = np.einsum("pqkBb,hj->Bhqbpjk", turn, np.eye(4))
    return split_table(full.reshape(256, 256))


def dot(a, b):
    return lax.dot_general(a, b, (((1,), (0,)), ((), ())), preferred_element_type=F32)


def prepare_kernel(*refs):
    @pl.when(lax.axis_index(COL) == 0)
    def _():
        prepare_rows(lax.axis_index(ROW), *refs)


def prepare_rows(row, *refs):
    sources, out_hbm, targets, (out_ref, sems) = refs[:4], refs[4], refs[5:9], refs[9:]
    sources = (sources[0], sources[1], sources[2].at[:, :1024], sources[3].at[:, :1024])
    copies = [
        pltpu.make_async_copy(source, target, sems.at[k])
        for k, (source, target) in enumerate(zip(sources, targets))
    ]
    for copy in copies:
        copy.start()
    for copy in copies:
        copy.wait()
    occ_decay_ref, vir_decay_ref, occ_ref, vir_ref = targets

    def column(decay_ref, count):
        index = lax.broadcasted_iota(jnp.int32, (count, 128), 0)
        out = jnp.zeros((count, 128), F32)
        for i in range(count):
            out = jnp.where(index == i, decay_ref[row * count + i], out)
        return out

    def scaled_tiles(ref, decay):
        tiles = [ref[:, 128 * t : 128 * (t + 1)].astype(F32) * decay for t in range(8)]
        return [
            [
                jnp.concatenate(
                    [tiles[4 * t + u][:, 32 * kind : 32 * (kind + 1)] for u in range(4)], axis=1
                )
                for kind in range(4)
            ]
            for t in range(2)
        ]

    occ = scaled_tiles(occ_ref, column(occ_decay_ref, 32))
    vir = scaled_tiles(vir_ref, column(vir_decay_ref, 16))
    for y1 in range(2):
        for t in range(2):
            for kind in range(4):
                piece = jnp.concatenate(
                    [
                        occ[t][kind][8 * y1 : 8 * (y1 + 1)],
                        occ[t][kind][8 * (2 + y1) : 8 * (3 + y1)],
                        vir[t][kind][8 * y1 : 8 * (y1 + 1)],
                    ],
                    axis=0,
                ).astype(BF16)
                for xl in range(2):
                    out_ref[4 * xl + 2 * y1 + t, kind] = piece
    result = pltpu.make_async_copy(out_ref, out_hbm, sems.at[4])
    result.start()
    result.wait()


def prepare(occ_decay, vir_decay, occ, vir):
    hbm = pl.BlockSpec(memory_space=pl.ANY)
    return pl.pallas_call(
        prepare_kernel,
        out_shape=jax.ShapeDtypeStruct((8, 4, 24, 128), BF16),
        in_specs=[hbm] * 4,
        out_specs=hbm,
        scratch_shapes=[
            pltpu.SMEM((1024,), F32),
            pltpu.SMEM((512,), F32),
            pltpu.VMEM((32, 1024), BF16),
            pltpu.VMEM((16, 1024), BF16),
            pltpu.VMEM((8, 4, 24, 128), BF16),
            pltpu.SemaphoreType.DMA((5,)),
        ],
        name="prepare",
    )(occ_decay, vir_decay, occ, vir)


def pack_kernel(occ_ref, vir_ref, rows_ref, out_ref):
    for p in range(32):
        out_ref[p, 0:32, :] = occ_ref[:, 128 * p : 128 * (p + 1)]
        out_ref[p, 32:48, :] = vir_ref[:, 128 * p : 128 * (p + 1)]
        out_ref[p, 48:72, :] = rows_ref[0, p % 4]


def pack(occ, vir, rows):
    vmem = pl.BlockSpec(memory_space=pltpu.VMEM)
    return pl.pallas_call(
        pack_kernel,
        out_shape=jax.ShapeDtypeStruct((32, 72, 128), BF16),
        in_specs=[vmem] * 3,
        out_specs=vmem,
        compiler_params=pltpu.CompilerParams(vmem_limit_bytes=LIMIT),
        name="pack",
    )(occ, vir, rows)


def polar_kernel(*refs):
    points, near, (high_ref, low_ref) = refs[:4], refs[4:8], refs[8:10]
    out_ref, polar_ref, occ_ref, vir_ref = refs[-4:]
    core, z0, y = (lax.axis_index(axes) for axes in ("c", "z0", Y))
    for step in range(4):
        chunk = lax.rem(y + 4 - step, 4)
        y1, y0 = lax.div(chunk, 2), lax.rem(chunk, 2)
        lanes = pl.ds(pl.multiple_of(128 * y0, 128), 128)

        def rows(group):
            return pl.ds(pl.multiple_of(256 * group, 256), 256)

        occ_ref[rows(y1), lanes] = near[step][:256]
        occ_ref[rows(2 + y1), lanes] = near[step][256:512]
        vir_ref[rows(y1), lanes] = near[step][512:]
    occ = jnp.concatenate([ref[:, :1024] for ref in points], axis=0)
    vir = jnp.concatenate([ref[:, 1024:] for ref in points], axis=0)
    product = dot(occ, occ_ref[...]) * dot(vir, vir_ref[...]) * POLAR_FACTOR
    for k in range(4):
        place = 2 * (z0 if k < 2 else 1 - z0) + (core if k % 2 == 0 else 1 - core)
        polar_ref[pl.ds(pl.multiple_of(128 * place, 128), 128), :] = product[
            128 * k : 128 * (k + 1)
        ]
    for half in range(2):
        polar = polar_ref[256 * half : 256 * (half + 1), :]
        polar_high = polar.astype(BF16)
        polar_low = (polar - polar_high.astype(F32)).astype(BF16)
        spectrum = (
            dot(high_ref[...], polar_high)
            + dot(high_ref[...], polar_low)
            + dot(low_ref[...], polar_high)
        ).astype(BF16)
        for m in range(8):
            pieces = [spectrum[128 * i : 128 * (i + 1), 32 * m : 32 * (m + 1)] for i in range(4)]
            message = jnp.concatenate(pieces, axis=1)
            for j in range(8):
                out_ref[place_in_last(m, j), half] = message[16 * j : 16 * (j + 1)]


def polar_messages(*arrays):
    vmem = pl.BlockSpec(memory_space=pltpu.VMEM)
    return pl.pallas_call(
        polar_kernel,
        out_shape=jax.ShapeDtypeStruct((64, 2, 16, 128), BF16),
        in_specs=[vmem] * 10,
        out_specs=vmem,
        scratch_shapes=[
            pltpu.VMEM((512, 256), F32),
            pltpu.VMEM((1024, 256), BF16),
            pltpu.VMEM((512, 256), BF16),
        ],
        compiler_params=pltpu.CompilerParams(vmem_limit_bytes=LIMIT),
        name="polar",
    )(*arrays)


def finish_kernel(x_ref, a_high_ref, a_low_ref, b_high_ref, b_low_ref, *refs):
    outs, parts, sems = refs[:2], refs[2:4], refs[4]
    x = jnp.concatenate(
        [
            jnp.concatenate(
                [x_ref[place_in_last(2 * k + block // 2, j), block % 2] for k in range(4) for j in range(8)],
                axis=0,
            )
            for block in range(4)
        ],
        axis=1,
    )
    planes = dot(a_high_ref[...], x) + dot(a_low_ref[...], x)
    copies = []
    for part in range(4):
        z = jnp.concatenate(
            [
                jnp.concatenate(
                    [
                        planes[64 * g : 64 * (g + 1), 128 * block : 128 * (block + 1)]
                        for block in range(4)
                    ],
                    axis=0,
                ).T
                for g in (2 * part, 2 * part + 1)
            ],
            axis=0,
        )
        z_high = z.astype(BF16)
        z_low = (z - z_high.astype(F32)).astype(BF16)
        out = (
            dot(z_high, b_high_ref[...])
            + dot(z_high, b_low_ref[...])
            + dot(z_low, b_high_ref[...])
        )
        for which in range(2):
            for g in range(2):
                for i in range(4):
                    rows = 128 * g + 32 * i
                    parts[which][:, i, 128 * (2 * part + g) : 128 * (2 * part + g + 1)] = out[
                        rows : rows + 32, 128 * which : 128 * (which + 1)
                    ]
            lanes = pl.ds(256 * part, 256)
            copy = pltpu.make_async_copy(
                parts[which].at[:, :, lanes], outs[which].at[:, :, lanes], sems.at[which, part]
            )
            copy.start()
            copies.append(copy)
    for copy in copies:
        copy.wait()


def finish(x, *tables):
    vmem = pl.BlockSpec(memory_space=pltpu.VMEM)
    hbm = pl.BlockSpec(memory_space=pl.ANY)
    shape = jax.ShapeDtypeStruct((32, 4, 1024), F32)
    return pl.pallas_call(
        finish_kernel,
        out_shape=(shape, shape),
        in_specs=[vmem] * 5,
        out_specs=(hbm, hbm),
        scratch_shapes=[
            pltpu.VMEM((32, 4, 1024), F32),
            pltpu.VMEM((32, 4, 1024), F32),
            pltpu.SemaphoreType.DMA((2, 4)),
        ],
        compiler_params=pltpu.CompilerParams(vmem_limit_bytes=LIMIT),
        name="finish",
    )(x, *tables)


def carry_kernel(*refs):
    count = len(refs) // 2
    for in_ref, out_ref in zip(refs[:count], refs[count:]):
        out_ref[...] = in_ref[...]


def carry(*arrays):
    vmem = pl.BlockSpec(memory_space=pltpu.VMEM)
    return pl.pallas_call(
        carry_kernel,
        out_shape=[jax.ShapeDtypeStruct(a.shape, a.dtype) for a in arrays],
        in_specs=[vmem] * len(arrays),
        out_specs=[vmem] * len(arrays),
        compiler_params=pltpu.CompilerParams(vmem_limit_bytes=LIMIT),
        name="carry",
    )(*arrays)


def turn_kernel(in_ref, out_ref):
    out_ref[...] = in_ref[...].T


def turn(x):
    vmem = pl.BlockSpec(memory_space=pltpu.VMEM)
    return pl.pallas_call(
        turn_kernel,
        out_shape=jax.ShapeDtypeStruct(x.shape[::-1], x.dtype),
        in_specs=[vmem],
        out_specs=vmem,
        compiler_params=pltpu.CompilerParams(vmem_limit_bytes=LIMIT),
        name="turn",
    )(x)


def fence(x):
    anywhere = pl.BlockSpec(memory_space=pl.ANY)
    return pl.pallas_call(
        lambda in_ref, out_ref: None,
        out_shape=jax.ShapeDtypeStruct(x.shape, x.dtype),
        in_specs=[anywhere],
        out_specs=anywhere,
        input_output_aliases={0: 0},
        compiler_params=pltpu.CompilerParams(vmem_limit_bytes=LIMIT),
        name="fence",
    )(x)


def shift(x, axes, count, by):
    return lax.ppermute(x, axes, [(i, (i + by) % count) for i in range(count)])


def swap(x, axis):
    return lax.ppermute(x, axis, [(0, 1), (1, 0)])


def body(occ, vir, occ_decay, vir_decay):
    scattered = lax.all_to_all(prepare(occ_decay, vir_decay, occ, vir), COL, 0, 0, tiled=True)
    arrived = lax.all_to_all(pack(occ, vir, scattered), ROW, 0, 0, tiled=True)

    def by_group(part, count):
        part = part.reshape(32, count, 8, 128)
        return jnp.transpose(part, (1, 0, 2, 3)).reshape(256 * count, 128)

    near = jnp.concatenate([by_group(arrived[:, 48:64], 2), by_group(arrived[:, 64:], 1)], axis=0)
    near = [near]
    for by in (1, 2, 3):
        near.append(shift(near[0], Y, 4, by))
    own = jnp.concatenate([by_group(arrived[:, :32], 4), by_group(arrived[:, 32:48], 2)], axis=0)
    own = turn(own)
    across = swap(own, "z0")
    beside = swap(own, "c")
    beside = fence(beside)
    opposite = swap(across, "c")
    points = (own, beside, across, opposite)
    messages = polar_messages(*points, *near, *c_table())

    received = lax.all_to_all(messages, LAST, 0, 0, tiled=True)
    tables = carry(*a_table(), *b_table())
    return finish(received, *tables)


def solution(mesh):
    fine = Mesh(mesh.devices.reshape((2,) * len(FINE)), FINE)
    return jax.shard_map(
        body,
        mesh=fine,
        in_specs=(P(ROW, COL), P(ROW, COL), P(), P()),
        out_specs=(P(ROW, COL, None), P(ROW, COL, None)),
        check_vma=False,
    )
```

```python
import math

import jax
import jax.numpy as jnp
import numpy as np
from jax import lax
from jax.experimental import pallas as pl
from jax.experimental.pallas import tpu as pltpu
from jax.sharding import Mesh, PartitionSpec as P


NOCC = 1024
NVIR = 512
NGRID = 32768
POLAR_FACTOR = -1.0 / math.sqrt(NOCC * NVIR)
NORMAL = 1.0 / math.sqrt(NGRID)
Z = ("z2", "z1", "z0")
Y = ("y1", "y0")
ROW = ("xh", *Z, "c")
COL = ("xl", *Y)
FINE = ROW + COL
LAST = ("z1", "xl", "y0", "z2", "xh", "y1")
BF16 = jnp.bfloat16
F32 = jnp.float32
LIMIT = 16 * 1024 * 1024


def place_in_last(m, j):
    bits = dict(zip(("xh", "z2", "z1"), ((m >> 2) & 1, (m >> 1) & 1, m & 1)))
    bits.update(zip(COL, ((j >> 2) & 1, (j >> 1) & 1, j & 1)))
    place = 0
    for axis in LAST:
        place = 2 * place + bits[axis]
    return place


def split_table(table):
    high = table.astype(np.float32).astype(jnp.bfloat16)
    low = (table - high.astype(np.float64)).astype(np.float32).astype(jnp.bfloat16)
    return high, low


def rotation(phase):
    cosine, sine = np.cos(phase), np.sin(phase)
    return np.array([[cosine, sine], [-sine, cosine]])


def c_table():
    kc = np.arange(32).reshape(8, 4)
    turn = rotation(2 * np.pi * (kc[..., None] * np.arange(32) % 32) / 32)[:, 0]
    full = np.einsum("pjic,bd->ijpbdc", turn, np.eye(8))
    return split_table(full.reshape(512, 256))


def a_table():
    ka = np.arange(32)
    turn = rotation(2 * np.pi * (ka[:, None] * ka[None, :] % 32) / 32)
    turn = turn.reshape(2, 2, 8, 4, 8, 4)
    full = np.einsum("pqghck,bd->ghpbkcqd", turn, np.eye(8))
    return split_table(full.reshape(512, 512))


def b_table():
    kb = np.arange(32)
    turn = rotation(2 * np.pi * (kb[:, None] * kb[None, :] % 32) / 32) * NORMAL
    turn = turn.reshape(2, 2, 32, 4, 8)
    full = np.einsum("pqkBb,hj->Bhqbpjk", turn, np.eye(4))
    return split_table(full.reshape(256, 256))


def dot(a, b):
    return lax.dot_general(a, b, (((1,), (0,)), ((), ())), preferred_element_type=F32)


def prepare_kernel(*refs):
    @pl.when(lax.axis_index(COL) == 0)
    def _():
        prepare_rows(lax.axis_index(ROW), *refs)


def prepare_rows(row, *refs):
    sources, out_hbm, targets, (out_ref, sems) = refs[:4], refs[4], refs[5:9], refs[9:]
    sources = (sources[0], sources[1], sources[2].at[:, :1024], sources[3].at[:, :1024])
    copies = [
        pltpu.make_async_copy(source, target, sems.at[k])
        for k, (source, target) in enumerate(zip(sources, targets))
    ]
    for copy in copies:
        copy.start()
    for copy in copies:
        copy.wait()
    occ_decay_ref, vir_decay_ref, occ_ref, vir_ref = targets

    def column(decay_ref, count):
        index = lax.broadcasted_iota(jnp.int32, (count, 128), 0)
        out = jnp.zeros((count, 128), F32)
        for i in range(count):
            out = jnp.where(index == i, decay_ref[row * count + i], out)
        return out

    def scaled_tiles(ref, decay):
        tiles = [ref[:, 128 * t : 128 * (t + 1)].astype(F32) * decay for t in range(8)]
        return [
            [
                jnp.concatenate(
                    [tiles[4 * t + u][:, 32 * kind : 32 * (kind + 1)] for u in range(4)], axis=1
                )
                for kind in range(4)
            ]
            for t in range(2)
        ]

    occ = scaled_tiles(occ_ref, column(occ_decay_ref, 32))
    vir = scaled_tiles(vir_ref, column(vir_decay_ref, 16))
    for y1 in range(2):
        for t in range(2):
            for kind in range(4):
                piece = jnp.concatenate(
                    [
                        occ[t][kind][8 * y1 : 8 * (y1 + 1)],
                        occ[t][kind][8 * (2 + y1) : 8 * (3 + y1)],
                        vir[t][kind][8 * y1 : 8 * (y1 + 1)],
                    ],
                    axis=0,
                ).astype(BF16)
                for xl in range(2):
                    out_ref[4 * xl + 2 * y1 + t, kind] = piece
    result = pltpu.make_async_copy(out_ref, out_hbm, sems.at[4])
    result.start()
    result.wait()


def prepare(occ_decay, vir_decay, occ, vir):
    hbm = pl.BlockSpec(memory_space=pl.ANY)
    return pl.pallas_call(
        prepare_kernel,
        out_shape=jax.ShapeDtypeStruct((8, 4, 24, 128), BF16),
        in_specs=[hbm] * 4,
        out_specs=hbm,
        scratch_shapes=[
            pltpu.SMEM((1024,), F32),
            pltpu.SMEM((512,), F32),
            pltpu.VMEM((32, 1024), BF16),
            pltpu.VMEM((16, 1024), BF16),
            pltpu.VMEM((8, 4, 24, 128), BF16),
            pltpu.SemaphoreType.DMA((5,)),
        ],
        name="prepare",
    )(occ_decay, vir_decay, occ, vir)


def pack_kernel(occ_ref, vir_ref, rows_ref, out_ref):
    for p in range(32):
        out_ref[p, 0:32, :] = occ_ref[:, 128 * p : 128 * (p + 1)]
        out_ref[p, 32:48, :] = vir_ref[:, 128 * p : 128 * (p + 1)]
        out_ref[p, 48:72, :] = rows_ref[0, p % 4]


def pack(occ, vir, rows):
    vmem = pl.BlockSpec(memory_space=pltpu.VMEM)
    return pl.pallas_call(
        pack_kernel,
        out_shape=jax.ShapeDtypeStruct((32, 72, 128), BF16),
        in_specs=[vmem] * 3,
        out_specs=vmem,
        compiler_params=pltpu.CompilerParams(vmem_limit_bytes=LIMIT),
        name="pack",
    )(occ, vir, rows)


def polar_kernel(*refs):
    points, near, (high_ref, low_ref) = refs[:4], refs[4:8], refs[8:10]
    out_ref, polar_ref, occ_ref, vir_ref = refs[-4:]
    core, z0, y = (lax.axis_index(axes) for axes in ("c", "z0", Y))
    for step in range(4):
        chunk = lax.rem(y + 4 - step, 4)
        y1, y0 = lax.div(chunk, 2), lax.rem(chunk, 2)
        lanes = pl.ds(pl.multiple_of(128 * y0, 128), 128)

        def rows(group):
            return pl.ds(pl.multiple_of(256 * group, 256), 256)

        occ_ref[rows(y1), lanes] = near[step][:256]
        occ_ref[rows(2 + y1), lanes] = near[step][256:512]
        vir_ref[rows(y1), lanes] = near[step][512:]
    occ = jnp.concatenate([ref[:, :1024] for ref in points], axis=0)
    vir = jnp.concatenate([ref[:, 1024:] for ref in points], axis=0)
    product = dot(occ, occ_ref[...]) * dot(vir, vir_ref[...]) * POLAR_FACTOR
    for k in range(4):
        place = 2 * (z0 if k < 2 else 1 - z0) + (core if k % 2 == 0 else 1 - core)
        polar_ref[pl.ds(pl.multiple_of(128 * place, 128), 128), :] = product[
            128 * k : 128 * (k + 1)
        ]
    for half in range(2):
        polar = polar_ref[256 * half : 256 * (half + 1), :]
        polar_high = polar.astype(BF16)
        polar_low = (polar - polar_high.astype(F32)).astype(BF16)
        spectrum = (
            dot(high_ref[...], polar_high)
            + dot(high_ref[...], polar_low)
            + dot(low_ref[...], polar_high)
        ).astype(BF16)
        for m in range(8):
            pieces = [spectrum[128 * i : 128 * (i + 1), 32 * m : 32 * (m + 1)] for i in range(4)]
            message = jnp.concatenate(pieces, axis=1)
            for j in range(8):
                out_ref[place_in_last(m, j), half] = message[16 * j : 16 * (j + 1)]


def polar_messages(*arrays):
    vmem = pl.BlockSpec(memory_space=pltpu.VMEM)
    return pl.pallas_call(
        polar_kernel,
        out_shape=jax.ShapeDtypeStruct((64, 2, 16, 128), BF16),
        in_specs=[vmem] * 10,
        out_specs=vmem,
        scratch_shapes=[
            pltpu.VMEM((512, 256), F32),
            pltpu.VMEM((1024, 256), BF16),
            pltpu.VMEM((512, 256), BF16),
        ],
        compiler_params=pltpu.CompilerParams(vmem_limit_bytes=LIMIT),
        name="polar",
    )(*arrays)


def finish_kernel(x_ref, a_ref, b_high_ref, b_low_ref, *refs):
    outs, parts, sems = refs[:2], refs[2:4], refs[4]
    x = jnp.concatenate(
        [
            jnp.concatenate(
                [x_ref[place_in_last(2 * k + block // 2, j), block % 2] for k in range(4) for j in range(8)],
                axis=0,
            )
            for block in range(4)
        ],
        axis=1,
    )
    planes = dot(a_ref[...], x)
    copies = []
    for part in range(4):
        z = jnp.concatenate(
            [
                jnp.concatenate(
                    [
                        planes[64 * g : 64 * (g + 1), 128 * block : 128 * (block + 1)]
                        for block in range(4)
                    ],
                    axis=0,
                ).T
                for g in (2 * part, 2 * part + 1)
            ],
            axis=0,
        )
        z_high = z.astype(BF16)
        z_low = (z - z_high.astype(F32)).astype(BF16)
        out = (
            dot(z_high, b_high_ref[...])
            + dot(z_high, b_low_ref[...])
            + dot(z_low, b_high_ref[...])
        )
        for which in range(2):
            for g in range(2):
                for i in range(4):
                    rows = 128 * g + 32 * i
                    parts[which][:, i, 128 * (2 * part + g) : 128 * (2 * part + g + 1)] = out[
                        rows : rows + 32, 128 * which : 128 * (which + 1)
                    ]
            lanes = pl.ds(256 * part, 256)
            copy = pltpu.make_async_copy(
                parts[which].at[:, :, lanes], outs[which].at[:, :, lanes], sems.at[which, part]
            )
            copy.start()
            copies.append(copy)
    for copy in copies:
        copy.wait()


def finish(x, *tables):
    vmem = pl.BlockSpec(memory_space=pltpu.VMEM)
    hbm = pl.BlockSpec(memory_space=pl.ANY)
    shape = jax.ShapeDtypeStruct((32, 4, 1024), F32)
    return pl.pallas_call(
        finish_kernel,
        out_shape=(shape, shape),
        in_specs=[vmem] * 4,
        out_specs=(hbm, hbm),
        scratch_shapes=[
            pltpu.VMEM((32, 4, 1024), F32),
            pltpu.VMEM((32, 4, 1024), F32),
            pltpu.SemaphoreType.DMA((2, 4)),
        ],
        compiler_params=pltpu.CompilerParams(vmem_limit_bytes=LIMIT),
        name="finish",
    )(x, *tables)


def turn_kernel(in_ref, out_ref):
    out_ref[...] = in_ref[...].T


def turn(x):
    vmem = pl.BlockSpec(memory_space=pltpu.VMEM)
    return pl.pallas_call(
        turn_kernel,
        out_shape=jax.ShapeDtypeStruct(x.shape[::-1], x.dtype),
        in_specs=[vmem],
        out_specs=vmem,
        compiler_params=pltpu.CompilerParams(vmem_limit_bytes=LIMIT),
        name="turn",
    )(x)


def fence(x):
    anywhere = pl.BlockSpec(memory_space=pl.ANY)
    return pl.pallas_call(
        lambda in_ref, out_ref: None,
        out_shape=jax.ShapeDtypeStruct(x.shape, x.dtype),
        in_specs=[anywhere],
        out_specs=anywhere,
        input_output_aliases={0: 0},
        compiler_params=pltpu.CompilerParams(vmem_limit_bytes=LIMIT),
        name="fence",
    )(x)


def shift(x, axes, count, by):
    return lax.ppermute(x, axes, [(i, (i + by) % count) for i in range(count)])


def swap(x, axis):
    return lax.ppermute(x, axis, [(0, 1), (1, 0)])


def body(occ, vir, occ_decay, vir_decay):
    scattered = lax.all_to_all(prepare(occ_decay, vir_decay, occ, vir), COL, 0, 0, tiled=True)
    arrived = lax.all_to_all(pack(occ, vir, scattered), ROW, 0, 0, tiled=True)

    def by_group(part, count):
        part = part.reshape(32, count, 8, 128)
        return jnp.transpose(part, (1, 0, 2, 3)).reshape(256 * count, 128)

    near = jnp.concatenate([by_group(arrived[:, 48:64], 2), by_group(arrived[:, 64:], 1)], axis=0)
    near = [near]
    for by in (1, 2, 3):
        near.append(shift(near[0], Y, 4, by))
    own = jnp.concatenate([by_group(arrived[:, :32], 4), by_group(arrived[:, 32:48], 2)], axis=0)
    own = turn(own)
    across = swap(own, "z0")
    beside = swap(own, "c")
    beside = fence(beside)
    opposite = swap(across, "c")
    points = (own, beside, across, opposite)
    messages = polar_messages(*points, *near, *c_table())

    received = lax.all_to_all(messages, LAST, 0, 0, tiled=True)
    return finish(received, a_table()[0], *b_table())


def solution(mesh):
    fine = Mesh(mesh.devices.reshape((2,) * len(FINE)), FINE)
    return jax.shard_map(
        body,
        mesh=fine,
        in_specs=(P(ROW, COL), P(ROW, COL), P(), P()),
        out_specs=(P(ROW, COL, None), P(ROW, COL, None)),
        check_vma=False,
    )
```

```python
import math

import jax
import jax.numpy as jnp
import numpy as np
from jax import lax
from jax.experimental import pallas as pl
from jax.experimental.pallas import tpu as pltpu
from jax.sharding import Mesh, PartitionSpec as P


NOCC = 1024
NVIR = 512
NGRID = 32768
POLAR_FACTOR = -1.0 / math.sqrt(NOCC * NVIR) / math.sqrt(NGRID)
Z = ("z2", "z1", "z0")
Y = ("y1", "y0")
ROW = ("xh", *Z, "c")
COL = ("xl", *Y)
FINE = ROW + COL
LAST = ("z1", "xl", "y0", "z2", "xh", "y1")
BF16 = jnp.bfloat16
F32 = jnp.float32
LIMIT = 16 * 1024 * 1024


def place_in_last(m, j):
    bits = dict(zip(("xh", "z2", "z1"), ((m >> 2) & 1, (m >> 1) & 1, m & 1)))
    bits.update(zip(COL, ((j >> 2) & 1, (j >> 1) & 1, j & 1)))
    place = 0
    for axis in LAST:
        place = 2 * place + bits[axis]
    return place


def rotation(phase):
    cosine, sine = np.cos(phase), np.sin(phase)
    return np.array([[cosine, sine], [-sine, cosine]])


def c_table():
    kc = np.arange(32).reshape(8, 4)
    turn = rotation(2 * np.pi * (kc[..., None] * np.arange(32) % 32) / 32)[:, 0]
    full = np.einsum("pjic,bd->ijpbdc", turn, np.eye(8))
    return full.reshape(512, 256).astype(BF16)


def a_table():
    ka = np.arange(32)
    turn = rotation(2 * np.pi * (ka[:, None] * ka[None, :] % 32) / 32)
    turn = turn.reshape(2, 2, 8, 4, 8, 4)
    full = np.einsum("pqghck,bd->ghpbkcqd", turn, np.eye(8))
    return full.reshape(512, 512).astype(BF16)


def b_table():
    kb = np.arange(32)
    turn = rotation(2 * np.pi * (kb[:, None] * kb[None, :] % 32) / 32)
    turn = turn.reshape(2, 2, 32, 4, 8)
    full = np.einsum("pqkBb,hj->Bhqbpjk", turn, np.eye(4))
    return full.reshape(256, 256).astype(BF16)


def dot(a, b):
    return lax.dot_general(a, b, (((1,), (0,)), ((), ())), preferred_element_type=F32)


def prepare_kernel(*refs):
    @pl.when(lax.axis_index(COL) == 0)
    def _():
        prepare_rows(lax.axis_index(ROW), *refs)


def prepare_rows(row, *refs):
    sources, out_hbm, targets, (out_ref, sems) = refs[:4], refs[4], refs[5:9], refs[9:]
    sources = (sources[0], sources[1], sources[2].at[:, :1024], sources[3].at[:, :1024])
    copies = [
        pltpu.make_async_copy(source, target, sems.at[k])
        for k, (source, target) in enumerate(zip(sources, targets))
    ]
    for copy in copies:
        copy.start()
    for copy in copies:
        copy.wait()
    occ_decay_ref, vir_decay_ref, occ_ref, vir_ref = targets

    def column(decay_ref, count):
        index = lax.broadcasted_iota(jnp.int32, (count, 128), 0)
        out = jnp.zeros((count, 128), F32)
        for i in range(count):
            out = jnp.where(index == i, decay_ref[row * count + i], out)
        return out

    def scaled_tiles(ref, decay):
        tiles = [ref[:, 128 * t : 128 * (t + 1)].astype(F32) * decay for t in range(8)]
        return [
            [
                jnp.concatenate(
                    [tiles[4 * t + u][:, 32 * kind : 32 * (kind + 1)] for u in range(4)], axis=1
                )
                for kind in range(4)
            ]
            for t in range(2)
        ]

    occ = scaled_tiles(occ_ref, column(occ_decay_ref, 32))
    vir = scaled_tiles(vir_ref, column(vir_decay_ref, 16))
    for y1 in range(2):
        for t in range(2):
            for kind in range(4):
                piece = jnp.concatenate(
                    [
                        occ[t][kind][8 * y1 : 8 * (y1 + 1)],
                        occ[t][kind][8 * (2 + y1) : 8 * (3 + y1)],
                        vir[t][kind][8 * y1 : 8 * (y1 + 1)],
                    ],
                    axis=0,
                ).astype(BF16)
                for xl in range(2):
                    out_ref[4 * xl + 2 * y1 + t, kind] = piece
    result = pltpu.make_async_copy(out_ref, out_hbm, sems.at[4])
    result.start()
    result.wait()


def prepare(occ_decay, vir_decay, occ, vir):
    hbm = pl.BlockSpec(memory_space=pl.ANY)
    return pl.pallas_call(
        prepare_kernel,
        out_shape=jax.ShapeDtypeStruct((8, 4, 24, 128), BF16),
        in_specs=[hbm] * 4,
        out_specs=hbm,
        scratch_shapes=[
            pltpu.SMEM((1024,), F32),
            pltpu.SMEM((512,), F32),
            pltpu.VMEM((32, 1024), BF16),
            pltpu.VMEM((16, 1024), BF16),
            pltpu.VMEM((8, 4, 24, 128), BF16),
            pltpu.SemaphoreType.DMA((5,)),
        ],
        name="prepare",
    )(occ_decay, vir_decay, occ, vir)


def pack_kernel(occ_ref, vir_ref, rows_ref, out_ref):
    for p in range(32):
        out_ref[p, 0:32, :] = occ_ref[:, 128 * p : 128 * (p + 1)]
        out_ref[p, 32:48, :] = vir_ref[:, 128 * p : 128 * (p + 1)]
        out_ref[p, 48:72, :] = rows_ref[0, p % 4]


def pack(occ, vir, rows):
    vmem = pl.BlockSpec(memory_space=pltpu.VMEM)
    return pl.pallas_call(
        pack_kernel,
        out_shape=jax.ShapeDtypeStruct((32, 72, 128), BF16),
        in_specs=[vmem] * 3,
        out_specs=vmem,
        compiler_params=pltpu.CompilerParams(vmem_limit_bytes=LIMIT),
        name="pack",
    )(occ, vir, rows)


def polar_kernel(*refs):
    points, near, table_ref = refs[:4], refs[4:8], refs[8]
    out_ref, polar_ref, occ_ref, vir_ref = refs[-4:]
    core, z0, y = (lax.axis_index(axes) for axes in ("c", "z0", Y))
    for step in range(4):
        chunk = lax.rem(y + 4 - step, 4)
        y1, y0 = lax.div(chunk, 2), lax.rem(chunk, 2)
        lanes = pl.ds(pl.multiple_of(128 * y0, 128), 128)

        def rows(group):
            return pl.ds(pl.multiple_of(256 * group, 256), 256)

        occ_ref[rows(y1), lanes] = near[step][:256]
        occ_ref[rows(2 + y1), lanes] = near[step][256:512]
        vir_ref[rows(y1), lanes] = near[step][512:]
    occ = jnp.concatenate([ref[:, :1024] for ref in points], axis=0)
    vir = jnp.concatenate([ref[:, 1024:] for ref in points], axis=0)
    product = dot(occ, occ_ref[...]) * dot(vir, vir_ref[...]) * POLAR_FACTOR
    for k in range(4):
        place = 2 * (z0 if k < 2 else 1 - z0) + (core if k % 2 == 0 else 1 - core)
        polar_ref[pl.ds(pl.multiple_of(128 * place, 128), 128), :] = product[
            128 * k : 128 * (k + 1)
        ]
    for half in range(2):
        polar = polar_ref[256 * half : 256 * (half + 1), :]
        polar_high = polar.astype(BF16)
        polar_low = (polar - polar_high.astype(F32)).astype(BF16)
        spectrum = dot(table_ref[...], polar_high) + dot(table_ref[...], polar_low)
        spectrum = spectrum.astype(BF16)
        for m in range(8):
            pieces = [spectrum[128 * i : 128 * (i + 1), 32 * m : 32 * (m + 1)] for i in range(4)]
            message = jnp.concatenate(pieces, axis=1)
            for j in range(8):
                out_ref[place_in_last(m, j), half] = message[16 * j : 16 * (j + 1)]


def polar_messages(*arrays):
    vmem = pl.BlockSpec(memory_space=pltpu.VMEM)
    return pl.pallas_call(
        polar_kernel,
        out_shape=jax.ShapeDtypeStruct((64, 2, 16, 128), BF16),
        in_specs=[vmem] * 9,
        out_specs=vmem,
        scratch_shapes=[
            pltpu.VMEM((512, 256), F32),
            pltpu.VMEM((1024, 256), BF16),
            pltpu.VMEM((512, 256), BF16),
        ],
        compiler_params=pltpu.CompilerParams(vmem_limit_bytes=LIMIT),
        name="polar",
    )(*arrays)


def finish_kernel(x_ref, a_ref, b_ref, *refs):
    outs, parts, sems = refs[:2], refs[2:4], refs[4]
    x = jnp.concatenate(
        [
            jnp.concatenate(
                [x_ref[place_in_last(2 * k + block // 2, j), block % 2] for k in range(4) for j in range(8)],
                axis=0,
            )
            for block in range(4)
        ],
        axis=1,
    )
    planes = dot(a_ref[...], x)
    copies = []
    for part in range(4):
        z = jnp.concatenate(
            [
                jnp.concatenate(
                    [
                        planes[64 * g : 64 * (g + 1), 128 * block : 128 * (block + 1)]
                        for block in range(4)
                    ],
                    axis=0,
                ).T
                for g in (2 * part, 2 * part + 1)
            ],
            axis=0,
        )
        z_high = z.astype(BF16)
        z_low = (z - z_high.astype(F32)).astype(BF16)
        out = dot(z_high, b_ref[...]) + dot(z_low, b_ref[...])
        for which in range(2):
            for g in range(2):
                for i in range(4):
                    rows = 128 * g + 32 * i
                    parts[which][:, i, 128 * (2 * part + g) : 128 * (2 * part + g + 1)] = out[
                        rows : rows + 32, 128 * which : 128 * (which + 1)
                    ]
            lanes = pl.ds(256 * part, 256)
            copy = pltpu.make_async_copy(
                parts[which].at[:, :, lanes], outs[which].at[:, :, lanes], sems.at[which, part]
            )
            copy.start()
            copies.append(copy)
    for copy in copies:
        copy.wait()


def finish(x, *tables):
    vmem = pl.BlockSpec(memory_space=pltpu.VMEM)
    hbm = pl.BlockSpec(memory_space=pl.ANY)
    shape = jax.ShapeDtypeStruct((32, 4, 1024), F32)
    return pl.pallas_call(
        finish_kernel,
        out_shape=(shape, shape),
        in_specs=[vmem] * 3,
        out_specs=(hbm, hbm),
        scratch_shapes=[
            pltpu.VMEM((32, 4, 1024), F32),
            pltpu.VMEM((32, 4, 1024), F32),
            pltpu.SemaphoreType.DMA((2, 4)),
        ],
        compiler_params=pltpu.CompilerParams(vmem_limit_bytes=LIMIT),
        name="finish",
    )(x, *tables)


def turn_kernel(in_ref, out_ref):
    out_ref[...] = in_ref[...].T


def turn(x):
    vmem = pl.BlockSpec(memory_space=pltpu.VMEM)
    return pl.pallas_call(
        turn_kernel,
        out_shape=jax.ShapeDtypeStruct(x.shape[::-1], x.dtype),
        in_specs=[vmem],
        out_specs=vmem,
        compiler_params=pltpu.CompilerParams(vmem_limit_bytes=LIMIT),
        name="turn",
    )(x)


def fence(x):
    anywhere = pl.BlockSpec(memory_space=pl.ANY)
    return pl.pallas_call(
        lambda in_ref, out_ref: None,
        out_shape=jax.ShapeDtypeStruct(x.shape, x.dtype),
        in_specs=[anywhere],
        out_specs=anywhere,
        input_output_aliases={0: 0},
        compiler_params=pltpu.CompilerParams(vmem_limit_bytes=LIMIT),
        name="fence",
    )(x)


def shift(x, axes, count, by):
    return lax.ppermute(x, axes, [(i, (i + by) % count) for i in range(count)])


def swap(x, axis):
    return lax.ppermute(x, axis, [(0, 1), (1, 0)])


def body(occ, vir, occ_decay, vir_decay):
    scattered = lax.all_to_all(prepare(occ_decay, vir_decay, occ, vir), COL, 0, 0, tiled=True)
    arrived = lax.all_to_all(pack(occ, vir, scattered), ROW, 0, 0, tiled=True)

    def by_group(part, count):
        part = part.reshape(32, count, 8, 128)
        return jnp.transpose(part, (1, 0, 2, 3)).reshape(256 * count, 128)

    near = jnp.concatenate([by_group(arrived[:, 48:64], 2), by_group(arrived[:, 64:], 1)], axis=0)
    near = [near]
    for by in (1, 2, 3):
        near.append(shift(near[0], Y, 4, by))
    own = jnp.concatenate([by_group(arrived[:, :32], 4), by_group(arrived[:, 32:48], 2)], axis=0)
    own = turn(own)
    across = swap(own, "z0")
    beside = swap(own, "c")
    beside = fence(beside)
    opposite = swap(across, "c")
    points = (own, beside, across, opposite)
    messages = polar_messages(*points, *near, c_table())

    received = lax.all_to_all(messages, LAST, 0, 0, tiled=True)
    return finish(received, a_table(), b_table())


def solution(mesh):
    fine = Mesh(mesh.devices.reshape((2,) * len(FINE)), FINE)
    return jax.shard_map(
        body,
        mesh=fine,
        in_specs=(P(ROW, COL), P(ROW, COL), P(), P()),
        out_specs=(P(ROW, COL, None), P(ROW, COL, None)),
        check_vma=False,
    )
```
